32 devices in a mesh: seq: 4 (over x, core), level: 8 (over z, y).
Axes of the slice: x: 2, y: 2, z: 4, core: 2. Of those that a mesh axis runs over, the one named last changes fastest.
Arguments:
- states: float32 [32, 480, 64, 128], P('seq', 'level'), may hold values from -0.3 to 0.3
- xbc: bfloat16 [32, 8, 1792], P('seq', None, 'level'), may hold values from -1.796875 to 1.796875
- rates: float32 [32, 8, 24], P('seq'), may hold values from 0.02 to 0.8
- level_weights: float32 [32, 8, 480], P('seq', None, 'level'), may hold values from 0.1 to 1
- positions: int32 [32], P('seq'), may hold values from 0 to 1048567, as said below
- accepted: int32 [32], P('seq'), may hold values from 0 to 8
Outputs:
- outputs: bfloat16 [32, 8, 1536], P('seq', None, 'level')
- new_states: float32 [32, 480, 64, 128], P('seq', 'level')
- acceptance: float32 [], replicated
The draws below stay inside these ranges and needn't reach their ends.
Inputs may be any that keep to these rules, and one draw needn't show every extreme that they name: `positions`: p + 8 stays below 2**20.
All inputs are finite; a program needn't handle non-finite values.
Results may differ from the reference program's by a relative error of at most 0.0019.
Values may be sent and summed in bfloat16 or wider, within the bound.
No kernel may reach another device: no remote copies, remote signals or barrier semaphores. Data moves between devices by JAX's collectives and lax.ppermute only.
A program may use at most 128 MiB of HBM per device.

```python
import math
import jax
import jax.numpy as jnp
from jax import lax

H = 24
P_SIZE = 64
N = 128
L = 20
K = 8
SEQS = 32


def draw_positions(key, part):
    lowest_bit = (K - 1).bit_length()
    keys = jax.random.split(jax.random.fold_in(key, 7), 3)
    bit_power = jax.random.randint(keys[0], (SEQS,), lowest_bit, L, dtype=jnp.int32)
    step_back = jax.random.randint(keys[1], (SEQS,), 1, K + 1, dtype=jnp.int32)
    ceiling = jnp.left_shift(jnp.int32(1), L - bit_power)
    multiple = jax.random.randint(keys[2], (SEQS,), 1, ceiling, dtype=jnp.int32)
    return (multiple * jnp.left_shift(jnp.int32(1), bit_power) - step_back).astype(jnp.int32)


def place_ends(values, rng, smallest, high):
    shape = values.shape
    spot = [jax.random.randint(jax.random.fold_in(rng, axis), (), 0, shape[axis]) for axis in range(len(shape))]
    values = values.at[tuple(spot)].set(smallest)
    longest = shape.index(max(shape))
    spot[longest] = (spot[longest] + 1) % shape[longest]
    return values.at[tuple(spot)].set(high)


def shard_levels(key, shape, shards, least, high):
    def one(dim, shards_of):
        steps = jax.random.uniform(jax.random.fold_in(jax.random.fold_in(key, 6), dim), (shards_of,), jnp.float32, least / len(shards), high / len(shards))
        return jnp.repeat(jnp.exp(steps), shape[dim] // shards_of).reshape((-1,) + (1,) * (len(shape) - dim - 1))

    level = one(*shards[0])
    for cut in shards[1:]:
        level = level * one(*cut)
    return level


def gaussian(own_key, dims, scale, bound, shards=(), held_as=jnp.bfloat16):
    array = scale * jax.random.normal(own_key, dims, jnp.float32)
    if shards:
        array = array * shard_levels(own_key, dims, shards, -0.22, 0.18)
    return jnp.clip(array, -bound, bound).astype(held_as)


def setup_inputs(seed: int = 0) -> dict:
    arg_keys = jax.random.split(jax.random.key(seed), 7)
    states = gaussian(arg_keys[0], (SEQS, H * L, P_SIZE, N), 0.05, 0.3, ((0, 4), (1, 8)), jnp.float32)
    xbc = gaussian(arg_keys[1], (SEQS, K, H * P_SIZE + 2 * N), 0.3, 1.796875, ((0, 4), (2, 8)))
    rates = jnp.clip(jnp.exp(math.log(0.8) - 3.6888795 * jax.random.uniform(arg_keys[2], (SEQS, K, H), jnp.float32) ** shard_levels(arg_keys[2], (SEQS, K, H), ((0, 4),), -0.2, 0.2)), 0.02, 0.8)
    level_weights = jnp.clip(jnp.exp(math.log(1.0) - 2.3025851 * jax.random.uniform(arg_keys[3], (SEQS, K, H * L), jnp.float32) ** shard_levels(arg_keys[3], (SEQS, K, H * L), ((0, 4), (2, 8)), -0.2, 0.2)), 0.1, 1.0)
    positions = draw_positions(jax.random.fold_in(arg_keys[6], 71), 0)
    accepted = place_ends(jax.random.randint(arg_keys[5], (SEQS,), 0, K + 1), jax.random.fold_in(arg_keys[5], 1), 0, K).astype(jnp.int32)
    return dict(states=states, xbc=xbc, rates=rates, level_weights=level_weights, positions=positions, accepted=accepted)


def one_sequence(inputs_one):
    highest = lax.Precision.HIGHEST
    offset = L // 2
    block, drafts, decay_rates, weights_one, position, taken = inputs_one
    values = drafts[:, :H * P_SIZE].astype(jnp.float32).reshape(K, H, P_SIZE)
    in_vecs = drafts[:, H * P_SIZE:H * P_SIZE + N].astype(jnp.float32)
    out_vecs = drafts[:, H * P_SIZE + N:].astype(jnp.float32)
    cumul = jnp.cumsum(-decay_rates, axis=0)
    levels = jnp.arange(L, dtype=jnp.int32)
    occupied = (jnp.right_shift(position, levels) % 2).astype(jnp.float32)
    level_states = jnp.roll(block, offset, axis=0).reshape(H, L, P_SIZE, N)
    weights = jnp.roll(weights_one, offset, axis=1).reshape(K, H, L)
    readout = jnp.einsum('hlpn,tn->thlp', level_states, out_vecs, precision=highest)
    factor = weights * occupied[None, None, :] * jnp.exp(cumul)[:, :, None]
    from_states = jnp.sum(factor[..., None] * readout, axis=2)
    steps_all = jnp.arange(K, dtype=jnp.int32)
    causal = steps_all[None, :] <= steps_all[:, None]
    scores = jnp.dot(out_vecs, in_vecs.T, precision=highest)
    spread = cumul[:, None, :] - cumul[None, :, :]
    mixing = jnp.where(causal[:, :, None], jnp.exp(jnp.minimum(spread, 0.0)), 0.0) * scores[:, :, None]
    from_drafts = weights[:, :, 0][..., None] * jnp.einsum('tuh,uhp->thp', mixing, values, precision=highest)
    result = (from_states + from_drafts).reshape(K, H * P_SIZE).astype(jnp.bfloat16)
    new_position = position + taken
    new_occupied = (jnp.right_shift(new_position, levels) % 2).astype(jnp.float32)
    changed = jnp.bitwise_xor(position, new_position)
    top_level = jnp.sum((jnp.right_shift(changed, levels) > 0).astype(jnp.int32)) - 1
    staying = occupied * (levels > top_level).astype(jnp.float32)
    leaving = occupied * (levels < top_level).astype(jnp.float32)
    moved = jnp.sum(leaving[None, :, None, None] * level_states, axis=1)
    target = (levels == top_level).astype(jnp.float32)
    merged = staying[None, :, None, None] * level_states + target[None, :, None, None] * moved[:, None]
    live = (steps_all < taken).astype(jnp.float32)
    cum_taken = jnp.sum(-decay_rates * live[:, None], axis=0)
    token_pos = position + steps_all
    start_new = jnp.left_shift(jnp.right_shift(new_position, levels + 1), levels + 1)
    level_span = jnp.left_shift(jnp.int32(1), levels)
    inside = ((token_pos[None, :] >= start_new[:, None]) & (token_pos[None, :] < start_new[:, None] + level_span[:, None])).astype(jnp.float32) * live[None, :]
    token_decay = jnp.exp(jnp.minimum(cum_taken[None, :] - cumul, 0.0)) * live[:, None]
    tokens = jnp.einsum('lu,uh,uhp,un->hlpn', inside, token_decay, values, in_vecs, precision=highest)
    updated = new_occupied[None, :, None, None] * (jnp.exp(cum_taken)[:, None, None, None] * merged + tokens)
    return result, jnp.roll(updated.reshape(H * L, P_SIZE, N), -offset, axis=0)


def reference(states, xbc, rates, level_weights, positions, accepted):
    outputs, new_states = lax.map(one_sequence, (states, xbc, rates, level_weights, positions, accepted))
    acceptance = jnp.sum(accepted.astype(jnp.float32)) / (SEQS * K)
    return outputs, new_states, acceptance
```

```python
import functools

import jax
import jax.numpy as jnp
from jax import lax
from jax.experimental import pallas as pl
from jax.experimental.pallas import tpu as pltpu
from jax.sharding import PartitionSpec as P

H = 24
P_SIZE = 64
N = 128
L = 20
K = 8
VMEM = 24 * 2**20


def passed_along(x, axis, by):
    devices = lax.axis_size(axis)
    return lax.ppermute(x, axis, [(i, (i + by) % devices) for i in range(devices)])


def on_device(states, xbc, rates, level_weights, positions, accepted):
    highest = lax.Precision.HIGHEST
    seqs_local, local_count, width_p, width_n = states.shape
    offset = L // 2
    total_entries = H * L
    gathered = lax.all_gather(xbc, "level", axis=2, tiled=True).astype(jnp.float32)
    values = gathered[:, :, : H * P_SIZE].reshape(seqs_local, K, H, P_SIZE)
    in_vecs = gathered[:, :, H * P_SIZE : H * P_SIZE + N]
    out_vecs = gathered[:, :, H * P_SIZE + N :]
    cumul = jnp.cumsum(-rates, axis=1)
    first_entry = lax.axis_index("level") * local_count
    entries = first_entry + jnp.arange(local_count, dtype=jnp.int32)
    global_ids = (entries + offset) % total_entries
    head_of = global_ids // L
    level_of = global_ids % L
    head_ids = jnp.arange(H, dtype=jnp.int32)
    select = (head_of[:, None] == head_ids[None, :]).astype(jnp.float32)
    occupied = (jnp.right_shift(positions[:, None], level_of[None, :]) % 2).astype(jnp.float32)
    cum_local = jnp.einsum("sth,jh->stj", cumul, select, precision=highest)
    readout = jnp.einsum("sjpn,stn->stjp", states, out_vecs, precision=highest)
    factor = level_weights * occupied[:, None, :] * jnp.exp(cum_local)
    steps_all = jnp.arange(K, dtype=jnp.int32)
    causal = steps_all[None, :] <= steps_all[:, None]
    scores = jnp.einsum("stn,sun->stu", out_vecs, in_vecs, precision=highest)
    spread = cumul[:, :, None, :] - cumul[:, None, :, :]
    mixing = (
        jnp.where(causal[None, :, :, None], jnp.exp(jnp.minimum(spread, 0.0)), 0.0)
        * scores[..., None]
    )
    is_first = (level_of == 0).astype(jnp.float32)
    devices = lax.axis_size("level")
    own_width = H * P_SIZE // devices
    most_heads = 1
    distances = []
    for sender in range(devices):
        start_global = (sender * local_count + offset) % total_entries
        head_low = start_global // L
        head_count = (start_global + local_count - 1) // L - head_low + 1
        most_heads = max(most_heads, head_count)
        for slot_index in range(head_count):
            head_now = (head_low + slot_index) % H
            for receiver in range(
                head_now * P_SIZE // own_width, ((head_now + 1) * P_SIZE - 1) // own_width + 1
            ):
                gap = (receiver - sender) % devices
                if gap > devices // 2:
                    gap = gap - devices
                if gap != 0 and gap not in distances:
                    distances.append(gap)
    first_head = (first_entry + offset) % total_entries // L
    slot_heads = (first_head + jnp.arange(most_heads, dtype=jnp.int32)) % H
    select_slot = (head_of[:, None] == slot_heads[None, :]).astype(jnp.float32)
    pick_head = (head_ids[:, None] == slot_heads[None, :]).astype(jnp.float32)
    states_slot = jnp.einsum("stj,stjp,ji->stip", factor, readout, select_slot, precision=highest)
    weight_slot = jnp.einsum(
        "stj,ji->sti", level_weights, select_slot * is_first[:, None], precision=highest
    )
    mixing_slot = jnp.einsum("stuh,hi->stui", mixing, pick_head, precision=highest)
    values_slot = jnp.einsum("suhp,hi->suip", values, pick_head, precision=highest)
    drafts_slot = weight_slot[..., None] * jnp.einsum(
        "stui,suip->stip", mixing_slot, values_slot, precision=highest
    )
    flat_slot = (states_slot + drafts_slot).reshape(seqs_local, K, most_heads * P_SIZE)

    def toward(distance):
        receiver_now = (lax.axis_index("level") + distance) % devices
        feature_ids = receiver_now * own_width + jnp.arange(own_width, dtype=jnp.int32)
        slot_of = (feature_ids // P_SIZE - first_head) % H
        valid = (slot_of < most_heads).astype(jnp.float32)
        offsets = jnp.clip(slot_of * P_SIZE + feature_ids % P_SIZE, 0, most_heads * P_SIZE - 1)
        picked = jnp.take(flat_slot, offsets, axis=2)
        return picked * valid[None, None, :]

    summed = toward(0)
    for distance in distances:
        summed = summed + passed_along(toward(distance), "level", distance)
    outputs = summed.astype(jnp.bfloat16)
    new_position = positions + accepted
    levels_all = jnp.arange(L, dtype=jnp.int32)
    changed = jnp.bitwise_xor(positions, new_position)
    top_level = (
        jnp.sum(
            (jnp.right_shift(changed[:, None], levels_all[None, :]) > 0).astype(jnp.int32), axis=1
        )
        - 1
    )
    staying = occupied * (level_of[None, :] > top_level[:, None]).astype(jnp.float32)
    leaving = occupied * (level_of[None, :] < top_level[:, None]).astype(jnp.float32)
    target = (level_of[None, :] == top_level[:, None]).astype(jnp.float32)
    reach = min(devices - 1, (L - 2 + local_count) // local_count)
    same_head = (head_of[:, None] == head_of[None, :]).astype(jnp.float32)
    incoming = jnp.einsum("ab,sb,sbpn->sapn", same_head, leaving, states, precision=highest)
    place = target * (head_of == first_head).astype(jnp.float32)[None, :]
    for distance in range(1, reach + 1):
        receiver_start = (first_entry + distance * local_count + offset) % total_entries
        receiver_head = receiver_start // L
        target_global = receiver_head * L + top_level
        in_range = (
            (target_global >= receiver_start) & (target_global < receiver_start + local_count)
        ).astype(jnp.float32)
        pick_mask = (
            leaving * (head_of == receiver_head).astype(jnp.float32)[None, :] * in_range[:, None]
        )
        folded_sum = jnp.einsum("sj,sjpn->spn", pick_mask, states, precision=highest)
        received = passed_along(folded_sum.astype(jnp.bfloat16), "level", distance).astype(
            folded_sum.dtype
        )
        incoming = incoming + place[:, :, None, None] * received[:, None]
    merged = staying[:, :, None, None] * states + target[:, :, None, None] * incoming
    new_occ = (jnp.right_shift(new_position[:, None], level_of[None, :]) % 2).astype(jnp.float32)
    live = (steps_all[None, :] < accepted[:, None]).astype(jnp.float32)
    cum_taken = jnp.sum(-rates * live[:, :, None], axis=1)
    taken_local = jnp.einsum("sh,jh->sj", cum_taken, select, precision=highest)
    token_pos = positions[:, None] + steps_all[None, :]
    start_new = jnp.left_shift(
        jnp.right_shift(new_position[:, None], level_of[None, :] + 1), level_of[None, :] + 1
    )
    level_span = jnp.left_shift(jnp.int32(1), level_of)
    inside = (
        (token_pos[:, None, :] >= start_new[:, :, None])
        & (token_pos[:, None, :] < start_new[:, :, None] + level_span[None, :, None])
    ).astype(jnp.float32) * live[:, None, :]
    token_decay = jnp.exp(jnp.minimum(taken_local[:, None, :] - cum_local, 0.0)) * live[:, :, None]
    values_local = jnp.einsum("suhp,jh->sujp", values, select, precision=highest)
    tokens = jnp.einsum(
        "sju,suj,sujp,sun->sjpn", inside, token_decay, values_local, in_vecs, precision=highest
    )
    new_states = new_occ[:, :, None, None] * (
        jnp.exp(taken_local)[:, :, None, None] * merged + tokens
    )
    total_taken = lax.psum(jnp.sum(accepted.astype(jnp.float32)), "seq")
    acceptance = total_taken / (lax.axis_size("seq") * seqs_local * K)
    return (outputs, new_states, acceptance)


def highest_bit(value):
    return sum((jnp.right_shift(value, bit) > 0).astype(jnp.int32) for bit in range(L)) - 1


def split(value):
    high = value.astype(jnp.bfloat16)
    low = (value - high.astype(jnp.float32)).astype(jnp.bfloat16)
    return high, low


def dot_nt(left, right):
    return lax.dot_general(
        left, right, (((1,), (1,)), ((), ())), preferred_element_type=jnp.float32
    )


def weighted_queries(factor, out_vecs):
    high, low = split(factor * out_vecs)
    rows = jnp.concatenate([high, low], axis=0)
    return jnp.concatenate([rows, rows], axis=1)


class Plan:
    def __init__(self, devices, states, xbc, rates):
        self.seqs, self.count, self.width_p, self.width_n = states.shape
        self.steps = xbc.shape[1]
        self.shard = xbc.shape[2]
        self.heads = rates.shape[2]
        self.devices = devices
        self.offset = L // 2
        self.own = self.count // L
        self.slots = self.own + 1
        self.rows = self.seqs * self.steps
        self.low = (self.steps - 1).bit_length()
        self.starts = [0] + [L - self.offset + i * L for i in range(self.own)] + [self.count]
        self.value_width = self.heads * self.width_p

    def fits(self):
        return (
            self.count % L == 0
            and L - self.offset == self.offset
            and self.devices & (self.devices - 1) == 0
            and self.devices > 1
            and self.heads == self.own * self.devices
            and self.steps == 8
            and self.low <= self.offset
        )

    def levels(self, slot):
        first = self.offset if slot == 0 else 0
        return [(j, first + j - self.starts[slot]) for j in range(self.starts[slot], self.starts[slot + 1])]


def tables_kernel(plan, pos, acc, rates_ref, weights_ref, states_ref, factor_ref, taken_ref,
                  decay_ref, mix_ref, fold_ref, count_ref):
    rows, steps, seqs = plan.rows, plan.steps, plan.seqs
    first_head = lax.axis_index("level") * plan.own
    for s in range(seqs):
        p, q = pos[s], pos[s] + acc[s]
        top = highest_bit(jnp.bitwise_xor(p, q))
        leaving = jnp.where(top >= plan.offset, p, 0)
        total = None
        for k in range(plan.offset):
            bit = (jnp.right_shift(leaving, k) & 1) * (k < top).astype(jnp.int32)
            term = states_ref[s, k] * bit.astype(jnp.float32)
            total = term if total is None else total + term
        fold_ref[s] = total.astype(fold_ref.dtype)
    count_ref[...] = jnp.full(count_ref.shape, sum(acc[s] for s in range(seqs)).astype(jnp.float32))
    rate = rates_ref[...].reshape(rows, plan.heads)
    weight = weights_ref[...].reshape(rows, plan.count)
    row = lax.broadcasted_iota(jnp.int32, (rows, rows), 0)
    col = lax.broadcasted_iota(jnp.int32, (rows, rows), 1)
    same = row // steps == col // steps
    tri = same & (col <= row)
    row1 = lax.broadcasted_iota(jnp.int32, (rows, 1), 0)
    taken1 = jnp.zeros((rows, 1), jnp.int32)
    place1 = jnp.zeros((rows, 1), jnp.int32)
    for s in range(seqs):
        taken1 = jnp.where(row1 // steps == s, acc[s], taken1)
        place1 = jnp.where(row1 // steps == s, pos[s], place1)
    live = same & (col % steps < taken1)
    highest = lax.Precision.HIGHEST
    cum = -jnp.dot(tri.astype(jnp.float32), rate, precision=highest, preferred_element_type=jnp.float32)
    cum_taken = -jnp.dot(live.astype(jnp.float32), rate, precision=highest, preferred_element_type=jnp.float32)
    grown = jnp.exp(cum)
    grown_taken = jnp.exp(cum_taken)
    token = jnp.exp(jnp.minimum(cum_taken - cum, 0.0)) * (row1 % steps < taken1).astype(jnp.float32)
    head_lane = lax.broadcasted_iota(jnp.int32, (rows, plan.heads), 1)
    lane = lax.broadcasted_iota(jnp.int32, (rows, plan.count), 1)
    scale = None
    for i in range(plan.slots):
        hot = head_lane == lax.rem(first_head + i, plan.heads)

        def pick(values):
            return jnp.sum(jnp.where(hot, values, 0.0), axis=1, keepdims=True)

        taken_ref[i] = jnp.broadcast_to(pick(grown_taken), (rows, plan.width_n))
        decay_ref[i] = jnp.broadcast_to(pick(token), (rows, plan.width_p))
        wide = jnp.broadcast_to(pick(grown), (rows, plan.count))
        scale = wide if i == 0 else jnp.where(lane >= plan.starts[i], wide, scale)
        if i > 0:
            here = pick(cum)
            across = jnp.sum(jnp.where(row == col, here, 0.0), axis=0, keepdims=True)
            first = plan.starts[i]
            mix = jnp.where(tri, jnp.exp(jnp.minimum(here - across, 0.0)), 0.0)
            mix_ref[i - 1] = mix * weight[:, first : first + 1]
    occupied = jnp.right_shift(place1, (lane + plan.offset) % L) & 1
    factor_ref[...] = weight * occupied.astype(jnp.float32) * scale


def assemble_kernel(plan, pair_ref, *refs):
    *far_refs, states_ref, factor_ref, decay_ref, mix_ref = refs[: plan.devices // 2 - 1 + 4]
    in_ref, out_ref, token_ref, draft_ref, send_ref, all_ref = refs[plan.devices // 2 - 1 + 4 :]
    rows, shard = plan.rows, plan.shard
    me = lax.axis_index("level")
    for half, ref in enumerate([pair_ref, *far_refs]):
        for side in range(2):
            source = jnp.bitwise_xor(me, 2 * half + side)
            part = ref[side].astype(jnp.float32).reshape(rows, shard)
            all_ref[source] = part.astype(jnp.bfloat16)

    def features(first, width, pieces):
        k = lax.broadcasted_iota(jnp.int32, (shard, width), 0)
        c = lax.broadcasted_iota(jnp.int32, (shard, width), 1)
        total = None
        start = first // shard
        for piece in range(pieces):
            source = start + piece
            hot = (k + source * shard == c + first).astype(jnp.float32).astype(jnp.bfloat16)
            index = jnp.minimum(source, plan.devices - 1)
            term = jnp.dot(all_ref[index], hot, preferred_element_type=jnp.float32)
            total = term if total is None else total + term
        return total

    def pieces_of(width):
        return (width + shard - 2) // shard + 1

    in_vecs = features(plan.value_width, plan.width_n, pieces_of(plan.width_n))
    out_vecs = features(plan.value_width + plan.width_n, plan.width_n, pieces_of(plan.width_n))
    in_ref[...] = in_vecs
    out_ref[...] = out_vecs
    scores = dot_nt(out_vecs.astype(jnp.bfloat16), in_vecs.astype(jnp.bfloat16))
    drafts = []
    for i in range(plan.slots):
        head = lax.rem(me * plan.own + i, plan.heads)
        value = features(head * plan.width_p, plan.width_p, pieces_of(plan.width_p))
        token_ref[:, i * plan.width_p : (i + 1) * plan.width_p] = value * decay_ref[i]
        if i > 0:
            high, low = split(mix_ref[i - 1] * scores)
            value = value.astype(jnp.bfloat16)
            drafts.append(
                jnp.dot(high, value, preferred_element_type=jnp.float32)
                + jnp.dot(low, value, preferred_element_type=jnp.float32)
            )
        else:
            drafts.append(jnp.zeros((rows, plan.width_p), jnp.float32))
    draft_ref[...] = jnp.concatenate(drafts[:-1], axis=1)
    steps = plan.steps
    for s in range(plan.seqs):
        at = slice(s * steps, (s + 1) * steps)
        query = out_vecs[at]
        total = None
        for k, (j, _) in enumerate(plan.levels(plan.own)):
            left = weighted_queries(factor_ref[at, j : j + 1], query)
            right = jnp.concatenate(split(states_ref[s, k]), axis=1)
            term = dot_nt(left, right)
            total = term if total is None else total + term
        send_ref[at] = total[:steps] + total[steps:] + drafts[-1][at]


def states_kernel(plan, pos, acc, states_ref, factor_ref, taken_ref, in_ref, out_ref, token_ref,
                  draft_ref, fold_ref, new_ref, own_ref):
    s = pl.program_id(0)
    steps, width_p, width_n = plan.steps, plan.width_p, plan.width_n
    p = pos[s]
    a = acc[s]
    q = p + a
    top = highest_bit(jnp.bitwise_xor(p, q))
    bound = jnp.maximum(top, 0)
    below = jnp.left_shift(1, bound) - 1
    upto = jnp.where(top < 0, 0, jnp.left_shift(2, bound) - 1)
    staying = p & q & jnp.bitwise_not(upto)
    leaving = jnp.where(top < 0, 0, p & below)
    step = lax.broadcasted_iota(jnp.int32, (2 * steps, width_n), 0) % steps
    in_vecs = in_ref[...]
    in_twice = jnp.concatenate([in_vecs, in_vecs], axis=0)
    groups = []
    for g in range(plan.low + 1):
        level = bound if g == plan.low else g
        wanted = (jnp.right_shift(q, level) & 1) == 1
        if g < plan.low:
            wanted = wanted & (top != g)
        start = jnp.left_shift(jnp.right_shift(q, level + 1), level + 1)
        last = jnp.minimum(start + jnp.left_shift(1, level) - p, a)
        last = jnp.where(wanted, last, 0)
        inside = (step >= start - p) & (step < last)
        groups.append(jnp.where(inside, in_twice, 0.0).astype(jnp.bfloat16))
    spread = jnp.concatenate(split(token_ref[...]), axis=0)
    added = lax.dot_general(
        spread, jnp.concatenate(groups, axis=1), (((0,), (0,)), ((), ())),
        preferred_element_type=jnp.float32,
    )

    def tokens(i, g):
        return added[i * width_p : (i + 1) * width_p, g * width_n : (g + 1) * width_n]

    query = out_ref[...]
    for i in range(plan.slots):
        grown = taken_ref[i, 0:1, :]
        merged = None
        total = None
        for j, level in plan.levels(i):
            state = states_ref[0, j]
            kept = (jnp.right_shift(staying, level) & 1).astype(jnp.float32)
            new = state * (grown * kept)
            if level < plan.low:
                new = new + tokens(i, level)
            new_ref[0, j] = new
            left = (jnp.right_shift(leaving, level) & 1).astype(jnp.float32)
            term = state * left
            merged = term if merged is None else merged + term
            if i < plan.own:
                rows = weighted_queries(factor_ref[:, j : j + 1], query)
                term = dot_nt(rows, jnp.concatenate(split(state), axis=1))
                total = term if total is None else total + term
        if i < plan.own:
            at = slice(i * width_p, (i + 1) * width_p)
            own_ref[:, at] = total[:steps] + total[steps:] + draft_ref[:, at]
        base = plan.starts[i] - (plan.offset if i == 0 else 0)
        here = top >= 0
        if i == 0:
            here = top >= plan.offset
            merged = merged + fold_ref[0].astype(jnp.float32)
        if i == plan.own:
            here = here & (top < plan.offset)

        @pl.when(here)
        def _():
            new_ref[0, base + top] = merged * grown + tokens(i, plan.low)


def finish_kernel(plan, own_ref, received_ref, out_ref):
    width_p = plan.width_p
    own = own_ref[...]
    first = own[:, :width_p] + received_ref[...]
    total = jnp.concatenate([first, own[:, width_p:]], axis=1)
    out_ref[...] = total.reshape(out_ref.shape).astype(out_ref.dtype)


def summed_over(x, axis):
    devices = lax.axis_size(axis)
    if devices & (devices - 1):
        return lax.psum(x, axis)
    by = 1
    while by < devices:
        x = x + lax.ppermute(x, axis, [(i, i ^ by) for i in range(devices)])
        by *= 2
    return x


def whole(shape, index=None):
    zeros = (0,) * len(shape)
    return pl.BlockSpec(shape, lambda *_: index if index else zeros)


def fast_on_device(plan, states, xbc, rates, level_weights, positions, accepted):
    devices, seqs, steps, rows = plan.devices, plan.seqs, plan.steps, plan.rows
    count, slots, own = plan.count, plan.slots, plan.own
    width_p, width_n = plan.width_p, plan.width_n
    f32 = jnp.float32
    swap = lambda x, by: lax.ppermute(x, "level", [(i, i ^ by) for i in range(devices)])
    boundary = ((seqs, plan.offset, width_p, width_n), (0, count // plan.offset - 1, 0, 0))
    beside = swap(xbc, 1)
    factor, taken, decay, mix, fold, counted = pl.pallas_call(
        functools.partial(tables_kernel, plan),
        grid_spec=pltpu.PrefetchScalarGridSpec(
            num_scalar_prefetch=2, grid=(1,),
            in_specs=[whole(rates.shape), whole(level_weights.shape), whole(*boundary)],
            out_specs=[whole((rows, count)), whole((slots, rows, width_n)), whole((slots, rows, width_p)),
                       whole((own, rows, rows)), whole((seqs, width_p, width_n)), whole((8, 128))],
        ),
        out_shape=[
            jax.ShapeDtypeStruct((rows, count), f32),
            jax.ShapeDtypeStruct((slots, rows, width_n), f32),
            jax.ShapeDtypeStruct((slots, rows, width_p), f32),
            jax.ShapeDtypeStruct((own, rows, rows), f32),
            jax.ShapeDtypeStruct((seqs, width_p, width_n), jnp.bfloat16),
            jax.ShapeDtypeStruct((8, 128), f32),
        ],
        compiler_params=pltpu.CompilerParams(vmem_limit_bytes=VMEM),
        cost_estimate=pl.CostEstimate(flops=2_000_000, bytes_accessed=3_000_000, transcendentals=0),
        name="tables",
    )(positions, accepted, rates, level_weights, states)
    pair = jnp.stack([xbc, beside])
    far = [swap(pair, by) for by in range(2, devices, 2)]
    fold_in = passed_along(fold, "level", 1)
    in_vecs, out_vecs, token, draft, send = pl.pallas_call(
        functools.partial(assemble_kernel, plan),
        grid=(1,),
        in_specs=[whole(pair.shape)] * (1 + len(far)) + [
            whole(*boundary), whole(factor.shape), whole(decay.shape), whole(mix.shape)],
        out_specs=[whole((rows, width_n))] * 2 + [whole((rows, slots * width_p)), whole((rows, own * width_p)),
                                                  whole((rows, width_p))],
        out_shape=[jax.ShapeDtypeStruct((rows, width_n), f32)] * 2 + [
            jax.ShapeDtypeStruct((rows, slots * width_p), f32),
            jax.ShapeDtypeStruct((rows, own * width_p), f32),
            jax.ShapeDtypeStruct((rows, width_p), f32)],
        scratch_shapes=[pltpu.VMEM((devices, rows, plan.shard), jnp.bfloat16)],
        compiler_params=pltpu.CompilerParams(vmem_limit_bytes=VMEM),
        cost_estimate=pl.CostEstimate(flops=2_000_000, bytes_accessed=3_000_000, transcendentals=0),
        name="assemble",
    )(pair, *far, states, factor, decay, mix)
    received = passed_along(send, "level", 1)
    new_states, own_out = pl.pallas_call(
        functools.partial(states_kernel, plan),
        grid_spec=pltpu.PrefetchScalarGridSpec(
            num_scalar_prefetch=2, grid=(seqs,),
            in_specs=[
                pl.BlockSpec((1, count, width_p, width_n), lambda s, *_: (s, 0, 0, 0)),
                pl.BlockSpec((steps, count), lambda s, *_: (s, 0)),
                pl.BlockSpec((slots, steps, width_n), lambda s, *_: (0, s, 0)),
                pl.BlockSpec((steps, width_n), lambda s, *_: (s, 0)),
                pl.BlockSpec((steps, width_n), lambda s, *_: (s, 0)),
                pl.BlockSpec((steps, slots * width_p), lambda s, *_: (s, 0)),
                pl.BlockSpec((steps, own * width_p), lambda s, *_: (s, 0)),
                pl.BlockSpec((1, width_p, width_n), lambda s, *_: (s, 0, 0)),
            ],
            out_specs=[
                pl.BlockSpec((1, count, width_p, width_n), lambda s, *_: (s, 0, 0, 0)),
                pl.BlockSpec((steps, own * width_p), lambda s, *_: (s, 0)),
            ],
        ),
        out_shape=[
            jax.ShapeDtypeStruct(states.shape, f32),
            jax.ShapeDtypeStruct((rows, own * width_p), f32),
        ],
        compiler_params=pltpu.CompilerParams(vmem_limit_bytes=VMEM),
        cost_estimate=pl.CostEstimate(flops=20_000_000, bytes_accessed=32_000_000, transcendentals=0),
        name="commit",
    )(positions, accepted, states, factor, taken, in_vecs, out_vecs, token, draft, fold_in)
    outputs = pl.pallas_call(
        functools.partial(finish_kernel, plan),
        grid=(1,),
        in_specs=[whole((rows, own * width_p)), whole((rows, width_p))],
        out_specs=whole((seqs, steps, own * width_p)),
        out_shape=jax.ShapeDtypeStruct((seqs, steps, own * width_p), jnp.bfloat16),
        name="finish",
    )(own_out, received)
    counted = summed_over(counted, "seq")
    acceptance = counted[0, 0] / (lax.axis_size("seq") * seqs * steps)
    return outputs, new_states, acceptance


def dispatch(states, xbc, rates, level_weights, positions, accepted):
    plan = Plan(lax.axis_size("level"), states, xbc, rates)
    step = functools.partial(fast_on_device, plan) if plan.fits() else on_device
    return step(states, xbc, rates, level_weights, positions, accepted)


def solution(mesh):
    in_specs = (
        P("seq", "level", None, None),
        P("seq", None, "level"),
        P("seq", None, None),
        P("seq", None, "level"),
        P("seq"),
        P("seq"),
    )
    out_specs = (P("seq", None, "level"), P("seq", "level", None, None), P())
    return jax.shard_map(
        dispatch, mesh=mesh, in_specs=in_specs, out_specs=out_specs, check_vma=False
    )
```

```python
import functools

import jax
import jax.numpy as jnp
from jax import lax
from jax.experimental import pallas as pl
from jax.experimental.pallas import tpu as pltpu
from jax.sharding import PartitionSpec as P

H = 24
P_SIZE = 64
N = 128
L = 20
K = 8
PARTS = 2
VMEM = 24 * 2**20
BASE_VMEM = 40 * 2**20


def passed_along(x, axis, by):
    devices = lax.axis_size(axis)
    return lax.ppermute(x, axis, [(i, (i + by) % devices) for i in range(devices)])


def on_device(states, xbc, rates, level_weights, positions, accepted):
    highest = lax.Precision.HIGHEST
    seqs_local, local_count, width_p, width_n = states.shape
    offset = L // 2
    total_entries = H * L
    gathered = lax.all_gather(xbc, "level", axis=2, tiled=True).astype(jnp.float32)
    values = gathered[:, :, : H * P_SIZE].reshape(seqs_local, K, H, P_SIZE)
    in_vecs = gathered[:, :, H * P_SIZE : H * P_SIZE + N]
    out_vecs = gathered[:, :, H * P_SIZE + N :]
    cumul = jnp.cumsum(-rates, axis=1)
    first_entry = lax.axis_index("level") * local_count
    entries = first_entry + jnp.arange(local_count, dtype=jnp.int32)
    global_ids = (entries + offset) % total_entries
    head_of = global_ids // L
    level_of = global_ids % L
    head_ids = jnp.arange(H, dtype=jnp.int32)
    select = (head_of[:, None] == head_ids[None, :]).astype(jnp.float32)
    occupied = (jnp.right_shift(positions[:, None], level_of[None, :]) % 2).astype(jnp.float32)
    cum_local = jnp.einsum("sth,jh->stj", cumul, select, precision=highest)
    readout = jnp.einsum("sjpn,stn->stjp", states, out_vecs, precision=highest)
    factor = level_weights * occupied[:, None, :] * jnp.exp(cum_local)
    steps_all = jnp.arange(K, dtype=jnp.int32)
    causal = steps_all[None, :] <= steps_all[:, None]
    scores = jnp.einsum("stn,sun->stu", out_vecs, in_vecs, precision=highest)
    spread = cumul[:, :, None, :] - cumul[:, None, :, :]
    mixing = (
        jnp.where(causal[None, :, :, None], jnp.exp(jnp.minimum(spread, 0.0)), 0.0)
        * scores[..., None]
    )
    is_first = (level_of == 0).astype(jnp.float32)
    devices = lax.axis_size("level")
    own_width = H * P_SIZE // devices
    most_heads = 1
    distances = []
    for sender in range(devices):
        start_global = (sender * local_count + offset) % total_entries
        head_low = start_global // L
        head_count = (start_global + local_count - 1) // L - head_low + 1
        most_heads = max(most_heads, head_count)
        for slot_index in range(head_count):
            head_now = (head_low + slot_index) % H
            for receiver in range(
                head_now * P_SIZE // own_width, ((head_now + 1) * P_SIZE - 1) // own_width + 1
            ):
                gap = (receiver - sender) % devices
                if gap > devices // 2:
                    gap = gap - devices
                if gap != 0 and gap not in distances:
                    distances.append(gap)
    first_head = (first_entry + offset) % total_entries // L
    slot_heads = (first_head + jnp.arange(most_heads, dtype=jnp.int32)) % H
    select_slot = (head_of[:, None] == slot_heads[None, :]).astype(jnp.float32)
    pick_head = (head_ids[:, None] == slot_heads[None, :]).astype(jnp.float32)
    states_slot = jnp.einsum("stj,stjp,ji->stip", factor, readout, select_slot, precision=highest)
    weight_slot = jnp.einsum(
        "stj,ji->sti", level_weights, select_slot * is_first[:, None], precision=highest
    )
    mixing_slot = jnp.einsum("stuh,hi->stui", mixing, pick_head, precision=highest)
    values_slot = jnp.einsum("suhp,hi->suip", values, pick_head, precision=highest)
    drafts_slot = weight_slot[..., None] * jnp.einsum(
        "stui,suip->stip", mixing_slot, values_slot, precision=highest
    )
    flat_slot = (states_slot + drafts_slot).reshape(seqs_local, K, most_heads * P_SIZE)

    def toward(distance):
        receiver_now = (lax.axis_index("level") + distance) % devices
        feature_ids = receiver_now * own_width + jnp.arange(own_width, dtype=jnp.int32)
        slot_of = (feature_ids // P_SIZE - first_head) % H
        valid = (slot_of < most_heads).astype(jnp.float32)
        offsets = jnp.clip(slot_of * P_SIZE + feature_ids % P_SIZE, 0, most_heads * P_SIZE - 1)
        picked = jnp.take(flat_slot, offsets, axis=2)
        return picked * valid[None, None, :]

    summed = toward(0)
    for distance in distances:
        summed = summed + passed_along(toward(distance), "level", distance)
    outputs = summed.astype(jnp.bfloat16)
    new_position = positions + accepted
    levels_all = jnp.arange(L, dtype=jnp.int32)
    changed = jnp.bitwise_xor(positions, new_position)
    top_level = (
        jnp.sum(
            (jnp.right_shift(changed[:, None], levels_all[None, :]) > 0).astype(jnp.int32), axis=1
        )
        - 1
    )
    staying = occupied * (level_of[None, :] > top_level[:, None]).astype(jnp.float32)
    leaving = occupied * (level_of[None, :] < top_level[:, None]).astype(jnp.float32)
    target = (level_of[None, :] == top_level[:, None]).astype(jnp.float32)
    reach = min(devices - 1, (L - 2 + local_count) // local_count)
    same_head = (head_of[:, None] == head_of[None, :]).astype(jnp.float32)
    incoming = jnp.einsum("ab,sb,sbpn->sapn", same_head, leaving, states, precision=highest)
    place = target * (head_of == first_head).astype(jnp.float32)[None, :]
    for distance in range(1, reach + 1):
        receiver_start = (first_entry + distance * local_count + offset) % total_entries
        receiver_head = receiver_start // L
        target_global = receiver_head * L + top_level
        in_range = (
            (target_global >= receiver_start) & (target_global < receiver_start + local_count)
        ).astype(jnp.float32)
        pick_mask = (
            leaving * (head_of == receiver_head).astype(jnp.float32)[None, :] * in_range[:, None]
        )
        folded_sum = jnp.einsum("sj,sjpn->spn", pick_mask, states, precision=highest)
        received = passed_along(folded_sum.astype(jnp.bfloat16), "level", distance).astype(
            folded_sum.dtype
        )
        incoming = incoming + place[:, :, None, None] * received[:, None]
    merged = staying[:, :, None, None] * states + target[:, :, None, None] * incoming
    new_occ = (jnp.right_shift(new_position[:, None], level_of[None, :]) % 2).astype(jnp.float32)
    live = (steps_all[None, :] < accepted[:, None]).astype(jnp.float32)
    cum_taken = jnp.sum(-rates * live[:, :, None], axis=1)
    taken_local = jnp.einsum("sh,jh->sj", cum_taken, select, precision=highest)
    token_pos = positions[:, None] + steps_all[None, :]
    start_new = jnp.left_shift(
        jnp.right_shift(new_position[:, None], level_of[None, :] + 1), level_of[None, :] + 1
    )
    level_span = jnp.left_shift(jnp.int32(1), level_of)
    inside = (
        (token_pos[:, None, :] >= start_new[:, :, None])
        & (token_pos[:, None, :] < start_new[:, :, None] + level_span[None, :, None])
    ).astype(jnp.float32) * live[:, None, :]
    token_decay = jnp.exp(jnp.minimum(taken_local[:, None, :] - cum_local, 0.0)) * live[:, :, None]
    values_local = jnp.einsum("suhp,jh->sujp", values, select, precision=highest)
    tokens = jnp.einsum(
        "sju,suj,sujp,sun->sjpn", inside, token_decay, values_local, in_vecs, precision=highest
    )
    new_states = new_occ[:, :, None, None] * (
        jnp.exp(taken_local)[:, :, None, None] * merged + tokens
    )
    total_taken = lax.psum(jnp.sum(accepted.astype(jnp.float32)), "seq")
    acceptance = total_taken / (lax.axis_size("seq") * seqs_local * K)
    return (outputs, new_states, acceptance)


def highest_bit(value):
    return sum((jnp.right_shift(value, bit) > 0).astype(jnp.int32) for bit in range(L)) - 1


def split(value):
    high = value.astype(jnp.bfloat16)
    low = (value - high.astype(jnp.float32)).astype(jnp.bfloat16)
    return high, low


def dot_nt(left, right):
    return lax.dot_general(
        left, right, (((1,), (1,)), ((), ())), preferred_element_type=jnp.float32
    )


def applied(sums, queries):
    lane = lax.broadcasted_iota(jnp.int32, (sums.shape[1], queries.shape[0]), 1)
    total = None
    for t in range(queries.shape[0]):
        term = jnp.sum(sums[t] * queries[t : t + 1, :], axis=1, keepdims=True)
        total = jnp.broadcast_to(term, lane.shape) if t == 0 else jnp.where(lane == t, term, total)
    return total.T


class Plan:
    def __init__(self, devices, states, xbc, rates):
        self.seqs, self.count, self.width_p, self.width_n = states.shape
        self.steps = xbc.shape[1]
        self.shard = xbc.shape[2]
        self.heads = rates.shape[2]
        self.devices = devices
        self.offset = L // 2
        self.own = self.count // L
        self.slots = self.own + 1
        self.rows = self.seqs * self.steps
        self.low = (self.steps - 1).bit_length()
        self.starts = [0] + [L - self.offset + i * L for i in range(self.own)] + [self.count]
        self.value_width = self.heads * self.width_p

    def fits(self, groups):
        return (
            self.count % L == 0
            and L - self.offset == self.offset
            and self.devices & (self.devices - 1) == 0
            and self.devices > 1
            and self.heads == self.own * self.devices
            and self.steps == 8
            and groups >= 4
            and groups & (groups - 1) == 0
            and self.low <= self.offset
        )

    def levels(self, slot):
        first = self.offset if slot == 0 else 0
        return [(j, first + j - self.starts[slot]) for j in range(self.starts[slot], self.starts[slot + 1])]


def tables_kernel(plan, pos_hbm, acc_hbm, rates_hbm, weights_hbm, states_hbm, factor_ref, taken_ref,
                  decay_ref, mix_ref, fold_ref, count_ref, pos, acc, rates_ref, weights_ref, states_ref, sems, state_sems):
    copies = [
        pltpu.make_async_copy(source, target, sems.at[n])
        for n, (source, target) in enumerate(
            [(pos_hbm, pos), (acc_hbm, acc), (rates_hbm, rates_ref), (weights_hbm, weights_ref)]
        )
    ]
    state_copies = [
        pltpu.make_async_copy(
            states_hbm.at[s, pl.ds(plan.count - plan.offset, plan.offset)], states_ref.at[s], state_sems.at[s]
        )
        for s in range(plan.seqs)
    ]
    for copy in copies + state_copies:
        copy.start()
    for copy in copies:
        copy.wait()
    rows, steps, seqs = plan.rows, plan.steps, plan.seqs
    first_head = lax.axis_index("level") * plan.own
    count_ref[...] = jnp.full(count_ref.shape, sum(acc[s] for s in range(seqs)).astype(jnp.float32))
    rate = rates_ref[...].reshape(rows, plan.heads)
    weight = weights_ref[...].reshape(rows, plan.count)
    row = lax.broadcasted_iota(jnp.int32, (rows, rows), 0)
    col = lax.broadcasted_iota(jnp.int32, (rows, rows), 1)
    same = row // steps == col // steps
    tri = same & (col <= row)
    row1 = lax.broadcasted_iota(jnp.int32, (rows, 1), 0)
    taken1 = jnp.zeros((rows, 1), jnp.int32)
    place1 = jnp.zeros((rows, 1), jnp.int32)
    for s in range(seqs):
        taken1 = jnp.where(row1 // steps == s, acc[s], taken1)
        place1 = jnp.where(row1 // steps == s, pos[s], place1)
    live = same & (col % steps < taken1)
    highest = lax.Precision.HIGHEST
    cum = -jnp.dot(tri.astype(jnp.float32), rate, precision=highest, preferred_element_type=jnp.float32)
    cum_taken = -jnp.dot(live.astype(jnp.float32), rate, precision=highest, preferred_element_type=jnp.float32)
    grown = jnp.exp(cum)
    grown_taken = jnp.exp(cum_taken)
    token = jnp.exp(jnp.minimum(cum_taken - cum, 0.0)) * (row1 % steps < taken1).astype(jnp.float32)
    head_lane = lax.broadcasted_iota(jnp.int32, (rows, plan.heads), 1)
    lane = lax.broadcasted_iota(jnp.int32, (rows, plan.count), 1)
    scale = None
    for i in range(plan.slots):
        hot = head_lane == lax.rem(first_head + i, plan.heads)

        def pick(values):
            return jnp.sum(jnp.where(hot, values, 0.0), axis=1, keepdims=True)

        taken_ref[i] = jnp.broadcast_to(pick(grown_taken), (rows, plan.width_n))
        decay_ref[i] = jnp.broadcast_to(pick(token), (rows, plan.width_p))
        wide = jnp.broadcast_to(pick(grown), (rows, plan.count))
        scale = wide if i == 0 else jnp.where(lane >= plan.starts[i], wide, scale)
        if i > 0:
            here = pick(cum)
            across = jnp.sum(jnp.where(row == col, here, 0.0), axis=0, keepdims=True)
            first = plan.starts[i]
            mix = jnp.where(tri, jnp.exp(jnp.minimum(here - across, 0.0)), 0.0)
            mix_ref[i - 1] = mix * weight[:, first : first + 1]
    occupied = jnp.right_shift(place1, (lane + plan.offset) % L) & 1
    factor_ref[...] = weight * occupied.astype(jnp.float32) * scale
    for s in range(seqs):
        p, q = pos[s], pos[s] + acc[s]
        top = highest_bit(jnp.bitwise_xor(p, q))
        leaving = jnp.where(top >= plan.offset, p, 0)
        state_copies[s].wait()
        total = None
        for k in range(plan.offset):
            bit = (jnp.right_shift(leaving, k) & 1) * (k < top).astype(jnp.int32)
            term = states_ref[s, k] * bit.astype(jnp.float32)
            total = term if total is None else total + term
        fold_ref[s] = total.astype(fold_ref.dtype)


def assemble_kernel(plan, pair_ref, *refs):
    *far_refs, sums_ref, decay_ref, mix_ref, count_ref, counted_ref = refs[: plan.devices // 2 - 1 + 5]
    in_ref, out_ref, token_ref, draft_ref, send_ref, sum_ref, all_ref = refs[plan.devices // 2 - 1 + 5 :]
    sum_ref[...] = count_ref[...] + counted_ref[...]
    rows, shard = plan.rows, plan.shard
    me = lax.axis_index("level")
    for half, ref in enumerate([pair_ref, *far_refs]):
        for side in range(2):
            source = jnp.bitwise_xor(me, 2 * half + side)
            part = ref[side].astype(jnp.float32).reshape(rows, shard)
            all_ref[source] = part.astype(jnp.bfloat16)

    def features(first, width, pieces):
        k = lax.broadcasted_iota(jnp.int32, (shard, width), 0)
        c = lax.broadcasted_iota(jnp.int32, (shard, width), 1)
        total = None
        start = first // shard
        for piece in range(pieces):
            source = start + piece
            hot = (k + source * shard == c + first).astype(jnp.float32).astype(jnp.bfloat16)
            index = jnp.minimum(source, plan.devices - 1)
            term = jnp.dot(all_ref[index], hot, preferred_element_type=jnp.float32)
            total = term if total is None else total + term
        return total

    def pieces_of(width):
        return (width + shard - 2) // shard + 1

    in_vecs = features(plan.value_width, plan.width_n, pieces_of(plan.width_n))
    out_vecs = features(plan.value_width + plan.width_n, plan.width_n, pieces_of(plan.width_n))
    in_ref[...] = in_vecs
    out_ref[...] = out_vecs
    scores = dot_nt(out_vecs.astype(jnp.bfloat16), in_vecs.astype(jnp.bfloat16))
    drafts = []
    for i in range(plan.slots):
        head = lax.rem(me * plan.own + i, plan.heads)
        value = features(head * plan.width_p, plan.width_p, pieces_of(plan.width_p))
        token_ref[:, i * plan.width_p : (i + 1) * plan.width_p] = value * decay_ref[i]
        if i > 0:
            high, low = split(mix_ref[i - 1] * scores)
            value = value.astype(jnp.bfloat16)
            drafts.append(
                jnp.dot(high, value, preferred_element_type=jnp.float32)
                + jnp.dot(low, value, preferred_element_type=jnp.float32)
            )
        else:
            drafts.append(jnp.zeros((rows, plan.width_p), jnp.float32))
    draft_ref[...] = jnp.concatenate(drafts[:-1], axis=1)
    steps = plan.steps
    for s in range(plan.seqs):
        at = slice(s * steps, (s + 1) * steps)
        send_ref[at] = applied(sums_ref[s, plan.own], out_vecs[at]) + drafts[-1][at]


def base_kernel(plan, pos, acc, *refs):
    parts = plan.count // plan.offset
    states_refs = refs[:parts]
    factor_ref, taken_ref, new_hbm, sums_ref, low_ref, merged_ref, new_ref, wide_ref, sems = refs[parts:]
    s = pl.program_id(0)
    steps, width_p, width_n = plan.steps, plan.width_p, plan.width_n
    p = pos[s]
    q = p + acc[s]
    top = highest_bit(jnp.bitwise_xor(p, q))
    bound = jnp.maximum(top, 0)
    upto = jnp.where(top < 0, 0, jnp.left_shift(2, bound) - 1)
    staying = p & q & jnp.bitwise_not(upto)
    leaving = jnp.where(top < 0, 0, p & (jnp.left_shift(1, bound) - 1))
    side = lax.rem(s, 2)

    def sent(i, s, side):
        at = pl.ds(plan.starts[i], plan.starts[i + 1] - plan.starts[i])
        return pltpu.make_async_copy(new_ref.at[side, at], new_hbm.at[s, at], sems.at[side, i])

    for j in range(plan.count):
        wide_ref[j] = jnp.broadcast_to(factor_ref[:, j : j + 1], (steps, width_n))
    half = width_p // PARTS
    for i in range(plan.slots):

        @pl.when(s >= 2)
        def _():
            sent(i, s - 2, side).wait()

        grown = taken_ref[i, 0:1, :]
        for part in range(PARTS):
            at = slice(part * half, (part + 1) * half)
            sums = [None] * steps
            merged = None
            for j, level in plan.levels(i):
                state = states_refs[j // plan.offset][0, j % plan.offset, at, :]
                kept = (jnp.right_shift(staying, level) & 1).astype(jnp.float32)
                new = state * (grown * kept)
                new_ref[side, j, at, :] = new
                if level < plan.low:
                    low_ref[0, i - 1, level, at, :] = new
                left = (jnp.right_shift(leaving, level) & 1).astype(jnp.float32)
                term = state * left
                merged = term if merged is None else merged + term
                for t in range(steps):
                    term = state * wide_ref[j, t : t + 1, :]
                    sums[t] = term if sums[t] is None else sums[t] + term
            merged_ref[0, i, at, :] = merged
            for t in range(steps):
                sums_ref[0, i, t, at, :] = sums[t]
        sent(i, s, side).start()

    @pl.when(s == plan.seqs - 1)
    def _():
        for i in range(plan.slots):
            if plan.seqs > 1:
                sent(i, s - 1, 1 - side).wait()
            sent(i, s, side).wait()


def settle_kernel(plan, pos, acc, sums_ref, low_ref, merged_ref, taken_ref, in_ref, out_ref, token_ref,
                  draft_ref, fold_ref, old_hbm, new_hbm, own_ref, low_buf, top_buf, low_sems, top_sems):
    del old_hbm
    steps, width_p, width_n, low = plan.steps, plan.width_p, plan.width_n, plan.low
    step = lax.broadcasted_iota(jnp.int32, (2 * steps, width_n), 0) % steps
    copies = []
    for s in range(plan.seqs):
        rows = slice(s * steps, (s + 1) * steps)
        p = pos[s]
        a = acc[s]
        q = p + a
        top = highest_bit(jnp.bitwise_xor(p, q))
        bound = jnp.maximum(top, 0)
        in_vecs = in_ref[rows]
        in_twice = jnp.concatenate([in_vecs, in_vecs], axis=0)
        groups = []
        for g in range(low + 1):
            level = bound if g == low else g
            wanted = (jnp.right_shift(q, level) & 1) == 1
            if g < low:
                wanted = wanted & (top != g)
            start = jnp.left_shift(jnp.right_shift(q, level + 1), level + 1)
            last = jnp.minimum(start + jnp.left_shift(1, level) - p, a)
            last = jnp.where(wanted, last, 0)
            inside = (step >= start - p) & (step < last)
            groups.append(jnp.where(inside, in_twice, 0.0).astype(jnp.bfloat16))
        spread = jnp.concatenate(split(token_ref[rows]), axis=0)
        added = lax.dot_general(
            spread, jnp.concatenate(groups, axis=1), (((0,), (0,)), ((), ())),
            preferred_element_type=jnp.float32,
        )

        def tokens(i, g):
            return added[i * width_p : (i + 1) * width_p, g * width_n : (g + 1) * width_n]

        for i in range(plan.slots):
            grown = taken_ref[i, s * steps : s * steps + 1, :]
            merged = merged_ref[s, i]
            here = top >= 0
            if i == 0:
                here = top >= plan.offset
                merged = merged + fold_ref[s].astype(jnp.float32)
            if i == plan.own:
                here = here & (top < plan.offset)
            value = merged * grown + tokens(i, low)
            top_buf[s, i] = value
            base = plan.starts[i] - (plan.offset if i == 0 else 0)
            far = here & (top >= low)
            copy = pltpu.make_async_copy(
                top_buf.at[s, i], new_hbm.at[s, base + jnp.where(far, top, low)], top_sems.at[s, i]
            )
            copies.append((far, copy))
            pl.when(far)(copy.start)
            if i > 0:
                for g in range(low):
                    low_buf[s, i - 1, g] = low_ref[s, i - 1, g] + tokens(i, g)

                @pl.when(here & (top < low))
                def _():
                    low_buf[s, i - 1, bound] = value

                copy = pltpu.make_async_copy(
                    low_buf.at[s, i - 1], new_hbm.at[s, pl.ds(plan.starts[i], low)], low_sems.at[s, i - 1]
                )
                copies.append((None, copy))
                copy.start()
        query = out_ref[rows]
        for i in range(plan.own):
            at = slice(i * width_p, (i + 1) * width_p)
            own_ref[rows, at] = applied(sums_ref[s, i], query) + draft_ref[rows, at]
    for far, copy in copies:
        if far is None:
            copy.wait()
        else:
            pl.when(far)(copy.wait)


def finish_kernel(plan, scale, own_ref, received_ref, count_ref, counted_ref, out_ref, share_ref):
    width_p = plan.width_p
    own = own_ref[...]
    first = own[:, :width_p] + received_ref[...]
    total = jnp.concatenate([first, own[:, width_p:]], axis=1)
    out_ref[...] = total.reshape(out_ref.shape).astype(out_ref.dtype)
    share_ref[...] = ((count_ref[...] + counted_ref[...]) * scale)[:1, :1]


def whole(shape, index=None):
    zeros = (0,) * len(shape)
    return pl.BlockSpec(shape, lambda *_: index if index else zeros)


def fast_on_device(plan, states, xbc, rates, level_weights, positions, accepted):
    devices, seqs, steps, rows = plan.devices, plan.seqs, plan.steps, plan.rows
    count, slots, own = plan.count, plan.slots, plan.own
    width_p, width_n = plan.width_p, plan.width_n
    f32 = jnp.float32
    groups = lax.axis_size("seq")
    swap = lambda x, by: lax.ppermute(x, "level", [(i, i ^ by) for i in range(devices)])
    parts = count // plan.offset
    hbm = pl.BlockSpec(memory_space=pltpu.HBM)
    pair = jnp.stack([xbc, swap(xbc, 1)])
    far = [swap(pair, by) for by in range(2, devices, 2)]
    factor, taken, decay, mix, fold, counted = pl.pallas_call(
        functools.partial(tables_kernel, plan),
        grid=(1,),
        in_specs=[pl.BlockSpec(memory_space=pltpu.HBM)] * 5,
        out_specs=[whole((rows, count)), whole((slots, rows, width_n)), whole((slots, rows, width_p)),
                   whole((own, rows, rows)), whole((seqs, width_p, width_n)), whole((8, 128))],
        scratch_shapes=[
            pltpu.SMEM((seqs,), jnp.int32), pltpu.SMEM((seqs,), jnp.int32),
            pltpu.VMEM(rates.shape, f32), pltpu.VMEM(level_weights.shape, f32),
            pltpu.VMEM((seqs, plan.offset, width_p, width_n), f32),
            pltpu.SemaphoreType.DMA((4,)), pltpu.SemaphoreType.DMA((seqs,)),
        ],
        out_shape=[
            jax.ShapeDtypeStruct((rows, count), f32),
            jax.ShapeDtypeStruct((slots, rows, width_n), f32),
            jax.ShapeDtypeStruct((slots, rows, width_p), f32),
            jax.ShapeDtypeStruct((own, rows, rows), f32),
            jax.ShapeDtypeStruct((seqs, width_p, width_n), jnp.bfloat16),
            jax.ShapeDtypeStruct((8, 128), f32),
        ],
        compiler_params=pltpu.CompilerParams(vmem_limit_bytes=40 * 2**20),
        cost_estimate=pl.CostEstimate(flops=2_000_000, bytes_accessed=3_000_000, transcendentals=0),
        name="tables",
    )(*[pltpu.with_memory_space_constraint(x, pltpu.HBM) for x in (positions, accepted, rates, level_weights, states)])
    fold_in = passed_along(fold, "level", 1)
    base_states, sums, low, merged = pl.pallas_call(
        functools.partial(base_kernel, plan),
        grid_spec=pltpu.PrefetchScalarGridSpec(
            num_scalar_prefetch=2, grid=(seqs,),
            in_specs=[
                pl.BlockSpec((1, plan.offset, width_p, width_n), lambda s, *_, part=part: (s, part, 0, 0))
                for part in range(parts)
            ] + [
                pl.BlockSpec((steps, count), lambda s, *_: (s, 0)),
                pl.BlockSpec((slots, steps, width_n), lambda s, *_: (0, s, 0)),
            ],
            out_specs=[
                hbm,
                pl.BlockSpec((1, slots, steps, width_p, width_n), lambda s, *_: (s, 0, 0, 0, 0)),
                pl.BlockSpec((1, own, plan.low, width_p, width_n), lambda s, *_: (s, 0, 0, 0, 0)),
                pl.BlockSpec((1, slots, width_p, width_n), lambda s, *_: (s, 0, 0, 0)),
            ],
            scratch_shapes=[
                pltpu.VMEM((2, count, width_p, width_n), f32),
                pltpu.VMEM((count, steps, width_n), f32),
                pltpu.SemaphoreType.DMA((2, slots)),
            ],
        ),
        out_shape=[
            jax.ShapeDtypeStruct(states.shape, f32),
            jax.ShapeDtypeStruct((seqs, slots, steps, width_p, width_n), f32),
            jax.ShapeDtypeStruct((seqs, own, plan.low, width_p, width_n), f32),
            jax.ShapeDtypeStruct((seqs, slots, width_p, width_n), f32),
        ],
        compiler_params=pltpu.CompilerParams(vmem_limit_bytes=BASE_VMEM),
        cost_estimate=pl.CostEstimate(flops=20_000_000, bytes_accessed=32_000_000, transcendentals=0),
        name="base",
    )(positions, accepted, *[states] * parts, factor, taken)
    meet = lambda x, by: lax.ppermute(x, "seq", [(i, i ^ by) for i in range(groups)])
    counted_in = meet(counted, 1)
    in_vecs, out_vecs, token, draft, send, summed = pl.pallas_call(
        functools.partial(assemble_kernel, plan),
        grid=(1,),
        in_specs=[whole(pair.shape)] * (1 + len(far)) + [
            whole(sums.shape), whole(decay.shape), whole(mix.shape),
            whole(counted.shape), whole(counted.shape)],
        out_specs=[whole((rows, width_n))] * 2 + [whole((rows, slots * width_p)), whole((rows, own * width_p)),
                                                  whole((rows, width_p)), whole(counted.shape)],
        out_shape=[jax.ShapeDtypeStruct((rows, width_n), f32)] * 2 + [
            jax.ShapeDtypeStruct((rows, slots * width_p), f32),
            jax.ShapeDtypeStruct((rows, own * width_p), f32),
            jax.ShapeDtypeStruct((rows, width_p), f32),
            jax.ShapeDtypeStruct(counted.shape, f32)],
        scratch_shapes=[pltpu.VMEM((devices, rows, plan.shard), jnp.bfloat16)],
        compiler_params=pltpu.CompilerParams(vmem_limit_bytes=VMEM),
        cost_estimate=pl.CostEstimate(flops=2_000_000, bytes_accessed=3_000_000, transcendentals=0),
        name="assemble",
    )(pair, *far, sums, decay, mix, counted, counted_in)
    by = 2
    while 2 * by < groups:
        summed = summed + meet(summed, by)
        by *= 2
    summed_in = meet(summed, by)
    received = passed_along(send, "level", 1)
    settled = [whole(sums.shape), whole(low.shape), whole(merged.shape), whole(taken.shape),
               whole(in_vecs.shape), whole(out_vecs.shape), whole(token.shape), whole(draft.shape), whole(fold.shape)]
    new_states, own_out = pl.pallas_call(
        functools.partial(settle_kernel, plan),
        grid_spec=pltpu.PrefetchScalarGridSpec(
            num_scalar_prefetch=2, grid=(1,),
            in_specs=settled + [hbm],
            out_specs=[hbm, whole((rows, own * width_p))],
            scratch_shapes=[
                pltpu.VMEM(low.shape, f32), pltpu.VMEM(merged.shape, f32),
                pltpu.SemaphoreType.DMA((seqs, own)), pltpu.SemaphoreType.DMA((seqs, slots)),
            ],
        ),
        out_shape=[
            jax.ShapeDtypeStruct(states.shape, f32),
            jax.ShapeDtypeStruct((rows, own * width_p), f32),
        ],
        input_output_aliases={2 + len(settled): 0},
        compiler_params=pltpu.CompilerParams(vmem_limit_bytes=VMEM),
        cost_estimate=pl.CostEstimate(flops=8_000_000, bytes_accessed=8_000_000, transcendentals=0),
        name="settle",
    )(positions, accepted, sums, low, merged, taken, in_vecs, out_vecs, token, draft, fold_in, base_states)
    outputs, share = pl.pallas_call(
        functools.partial(finish_kernel, plan, 1.0 / (groups * seqs * steps)),
        grid=(1,),
        in_specs=[whole((rows, own * width_p)), whole((rows, width_p)), whole(counted.shape), whole(counted.shape)],
        out_specs=[whole((seqs, steps, own * width_p)), whole((1, 1))],
        out_shape=[jax.ShapeDtypeStruct((seqs, steps, own * width_p), jnp.bfloat16),
                   jax.ShapeDtypeStruct((1, 1), f32)],
        compiler_params=pltpu.CompilerParams(vmem_limit_bytes=VMEM),
        name="finish",
    )(own_out, received, summed, summed_in)
    return outputs, new_states, share.reshape(())


def dispatch(states, xbc, rates, level_weights, positions, accepted):
    plan = Plan(lax.axis_size("level"), states, xbc, rates)
    step = functools.partial(fast_on_device, plan) if plan.fits(lax.axis_size("seq")) else on_device
    return step(states, xbc, rates, level_weights, positions, accepted)


def solution(mesh):
    in_specs = (
        P("seq", "level", None, None),
        P("seq", None, "level"),
        P("seq", None, None),
        P("seq", None, "level"),
        P("seq"),
        P("seq"),
    )
    out_specs = (P("seq", None, "level"), P("seq", "level", None, None), P())
    return jax.shard_map(
        dispatch, mesh=mesh, in_specs=in_specs, out_specs=out_specs, check_vma=False
    )
```

```python
import functools

import jax
import jax.numpy as jnp
from jax import lax
from jax.experimental import pallas as pl
from jax.experimental.pallas import tpu as pltpu
from jax.sharding import PartitionSpec as P

H = 24
P_SIZE = 64
N = 128
L = 20
K = 8
PARTS = 4
VMEM = 24 * 2**20
BASE_VMEM = 20 * 2**20


def passed_along(x, axis, by):
    devices = lax.axis_size(axis)
    return lax.ppermute(x, axis, [(i, (i + by) % devices) for i in range(devices)])


def on_device(states, xbc, rates, level_weights, positions, accepted):
    highest = lax.Precision.HIGHEST
    seqs_local, local_count, width_p, width_n = states.shape
    offset = L // 2
    total_entries = H * L
    gathered = lax.all_gather(xbc, "level", axis=2, tiled=True).astype(jnp.float32)
    values = gathered[:, :, : H * P_SIZE].reshape(seqs_local, K, H, P_SIZE)
    in_vecs = gathered[:, :, H * P_SIZE : H * P_SIZE + N]
    out_vecs = gathered[:, :, H * P_SIZE + N :]
    cumul = jnp.cumsum(-rates, axis=1)
    first_entry = lax.axis_index("level") * local_count
    entries = first_entry + jnp.arange(local_count, dtype=jnp.int32)
    global_ids = (entries + offset) % total_entries
    head_of = global_ids // L
    level_of = global_ids % L
    head_ids = jnp.arange(H, dtype=jnp.int32)
    select = (head_of[:, None] == head_ids[None, :]).astype(jnp.float32)
    occupied = (jnp.right_shift(positions[:, None], level_of[None, :]) % 2).astype(jnp.float32)
    cum_local = jnp.einsum("sth,jh->stj", cumul, select, precision=highest)
    readout = jnp.einsum("sjpn,stn->stjp", states, out_vecs, precision=highest)
    factor = level_weights * occupied[:, None, :] * jnp.exp(cum_local)
    steps_all = jnp.arange(K, dtype=jnp.int32)
    causal = steps_all[None, :] <= steps_all[:, None]
    scores = jnp.einsum("stn,sun->stu", out_vecs, in_vecs, precision=highest)
    spread = cumul[:, :, None, :] - cumul[:, None, :, :]
    mixing = (
        jnp.where(causal[None, :, :, None], jnp.exp(jnp.minimum(spread, 0.0)), 0.0)
        * scores[..., None]
    )
    is_first = (level_of == 0).astype(jnp.float32)
    devices = lax.axis_size("level")
    own_width = H * P_SIZE // devices
    most_heads = 1
    distances = []
    for sender in range(devices):
        start_global = (sender * local_count + offset) % total_entries
        head_low = start_global // L
        head_count = (start_global + local_count - 1) // L - head_low + 1
        most_heads = max(most_heads, head_count)
        for slot_index in range(head_count):
            head_now = (head_low + slot_index) % H
            for receiver in range(
                head_now * P_SIZE // own_width, ((head_now + 1) * P_SIZE - 1) // own_width + 1
            ):
                gap = (receiver - sender) % devices
                if gap > devices // 2:
                    gap = gap - devices
                if gap != 0 and gap not in distances:
                    distances.append(gap)
    first_head = (first_entry + offset) % total_entries // L
    slot_heads = (first_head + jnp.arange(most_heads, dtype=jnp.int32)) % H
    select_slot = (head_of[:, None] == slot_heads[None, :]).astype(jnp.float32)
    pick_head = (head_ids[:, None] == slot_heads[None, :]).astype(jnp.float32)
    states_slot = jnp.einsum("stj,stjp,ji->stip", factor, readout, select_slot, precision=highest)
    weight_slot = jnp.einsum(
        "stj,ji->sti", level_weights, select_slot * is_first[:, None], precision=highest
    )
    mixing_slot = jnp.einsum("stuh,hi->stui", mixing, pick_head, precision=highest)
    values_slot = jnp.einsum("suhp,hi->suip", values, pick_head, precision=highest)
    drafts_slot = weight_slot[..., None] * jnp.einsum(
        "stui,suip->stip", mixing_slot, values_slot, precision=highest
    )
    flat_slot = (states_slot + drafts_slot).reshape(seqs_local, K, most_heads * P_SIZE)

    def toward(distance):
        receiver_now = (lax.axis_index("level") + distance) % devices
        feature_ids = receiver_now * own_width + jnp.arange(own_width, dtype=jnp.int32)
        slot_of = (feature_ids // P_SIZE - first_head) % H
        valid = (slot_of < most_heads).astype(jnp.float32)
        offsets = jnp.clip(slot_of * P_SIZE + feature_ids % P_SIZE, 0, most_heads * P_SIZE - 1)
        picked = jnp.take(flat_slot, offsets, axis=2)
        return picked * valid[None, None, :]

    summed = toward(0)
    for distance in distances:
        summed = summed + passed_along(toward(distance), "level", distance)
    outputs = summed.astype(jnp.bfloat16)
    new_position = positions + accepted
    levels_all = jnp.arange(L, dtype=jnp.int32)
    changed = jnp.bitwise_xor(positions, new_position)
    top_level = (
        jnp.sum(
            (jnp.right_shift(changed[:, None], levels_all[None, :]) > 0).astype(jnp.int32), axis=1
        )
        - 1
    )
    staying = occupied * (level_of[None, :] > top_level[:, None]).astype(jnp.float32)
    leaving = occupied * (level_of[None, :] < top_level[:, None]).astype(jnp.float32)
    target = (level_of[None, :] == top_level[:, None]).astype(jnp.float32)
    reach = min(devices - 1, (L - 2 + local_count) // local_count)
    same_head = (head_of[:, None] == head_of[None, :]).astype(jnp.float32)
    incoming = jnp.einsum("ab,sb,sbpn->sapn", same_head, leaving, states, precision=highest)
    place = target * (head_of == first_head).astype(jnp.float32)[None, :]
    for distance in range(1, reach + 1):
        receiver_start = (first_entry + distance * local_count + offset) % total_entries
        receiver_head = receiver_start // L
        target_global = receiver_head * L + top_level
        in_range = (
            (target_global >= receiver_start) & (target_global < receiver_start + local_count)
        ).astype(jnp.float32)
        pick_mask = (
            leaving * (head_of == receiver_head).astype(jnp.float32)[None, :] * in_range[:, None]
        )
        folded_sum = jnp.einsum("sj,sjpn->spn", pick_mask, states, precision=highest)
        received = passed_along(folded_sum.astype(jnp.bfloat16), "level", distance).astype(
            folded_sum.dtype
        )
        incoming = incoming + place[:, :, None, None] * received[:, None]
    merged = staying[:, :, None, None] * states + target[:, :, None, None] * incoming
    new_occ = (jnp.right_shift(new_position[:, None], level_of[None, :]) % 2).astype(jnp.float32)
    live = (steps_all[None, :] < accepted[:, None]).astype(jnp.float32)
    cum_taken = jnp.sum(-rates * live[:, :, None], axis=1)
    taken_local = jnp.einsum("sh,jh->sj", cum_taken, select, precision=highest)
    token_pos = positions[:, None] + steps_all[None, :]
    start_new = jnp.left_shift(
        jnp.right_shift(new_position[:, None], level_of[None, :] + 1), level_of[None, :] + 1
    )
    level_span = jnp.left_shift(jnp.int32(1), level_of)
    inside = (
        (token_pos[:, None, :] >= start_new[:, :, None])
        & (token_pos[:, None, :] < start_new[:, :, None] + level_span[None, :, None])
    ).astype(jnp.float32) * live[:, None, :]
    token_decay = jnp.exp(jnp.minimum(taken_local[:, None, :] - cum_local, 0.0)) * live[:, :, None]
    values_local = jnp.einsum("suhp,jh->sujp", values, select, precision=highest)
    tokens = jnp.einsum(
        "sju,suj,sujp,sun->sjpn", inside, token_decay, values_local, in_vecs, precision=highest
    )
    new_states = new_occ[:, :, None, None] * (
        jnp.exp(taken_local)[:, :, None, None] * merged + tokens
    )
    total_taken = lax.psum(jnp.sum(accepted.astype(jnp.float32)), "seq")
    acceptance = total_taken / (lax.axis_size("seq") * seqs_local * K)
    return (outputs, new_states, acceptance)


def highest_bit(value):
    return sum((jnp.right_shift(value, bit) > 0).astype(jnp.int32) for bit in range(L)) - 1


def split(value):
    high = value.astype(jnp.bfloat16)
    low = (value - high.astype(jnp.float32)).astype(jnp.bfloat16)
    return high, low


def dot_nt(left, right):
    return lax.dot_general(
        left, right, (((1,), (1,)), ((), ())), preferred_element_type=jnp.float32
    )


def applied(sums, queries):
    lane = lax.broadcasted_iota(jnp.int32, (sums.shape[1], queries.shape[0]), 1)
    total = None
    for t in range(queries.shape[0]):
        term = jnp.sum(sums[t] * queries[t : t + 1, :], axis=1, keepdims=True)
        total = jnp.broadcast_to(term, lane.shape) if t == 0 else jnp.where(lane == t, term, total)
    return total.T


class Plan:
    def __init__(self, devices, states, xbc, rates):
        self.seqs, self.count, self.width_p, self.width_n = states.shape
        self.steps = xbc.shape[1]
        self.shard = xbc.shape[2]
        self.heads = rates.shape[2]
        self.devices = devices
        self.offset = L // 2
        self.own = self.count // L
        self.slots = self.own + 1
        self.rows = self.seqs * self.steps
        self.low = (self.steps - 1).bit_length()
        self.starts = [0] + [L - self.offset + i * L for i in range(self.own)] + [self.count]
        self.value_width = self.heads * self.width_p

    def fits(self, groups):
        return (
            self.count % L == 0
            and L - self.offset == self.offset
            and self.devices & (self.devices - 1) == 0
            and self.devices > 1
            and self.heads == self.own * self.devices
            and self.steps == 8
            and self.seqs > 1
            and groups >= 4
            and groups & (groups - 1) == 0
            and self.low <= self.offset
        )

    def levels(self, slot):
        first = self.offset if slot == 0 else 0
        return [(j, first + j - self.starts[slot]) for j in range(self.starts[slot], self.starts[slot + 1])]


def tables_kernel(plan, pos_hbm, acc_hbm, rates_hbm, weights_hbm, states_hbm, factor_ref, taken_ref,
                  decay_ref, mix_ref, fold_ref, count_ref, pos, acc, rates_ref, weights_ref, states_ref, sems, state_sems):
    copies = [
        pltpu.make_async_copy(source, target, sems.at[n])
        for n, (source, target) in enumerate(
            [(pos_hbm, pos), (acc_hbm, acc), (rates_hbm, rates_ref), (weights_hbm, weights_ref)]
        )
    ]
    state_copies = [
        pltpu.make_async_copy(
            states_hbm.at[s, pl.ds(plan.count - plan.offset, plan.offset)], states_ref.at[s], state_sems.at[s]
        )
        for s in range(plan.seqs)
    ]
    for copy in copies + state_copies:
        copy.start()
    for copy in copies:
        copy.wait()
    rows, steps, seqs = plan.rows, plan.steps, plan.seqs
    first_head = lax.axis_index("level") * plan.own
    count_ref[...] = jnp.full(count_ref.shape, sum(acc[s] for s in range(seqs)).astype(jnp.float32))
    rate = rates_ref[...].reshape(rows, plan.heads)
    weight = weights_ref[...].reshape(rows, plan.count)
    row = lax.broadcasted_iota(jnp.int32, (rows, rows), 0)
    col = lax.broadcasted_iota(jnp.int32, (rows, rows), 1)
    same = row // steps == col // steps
    tri = same & (col <= row)
    row1 = lax.broadcasted_iota(jnp.int32, (rows, 1), 0)
    taken1 = jnp.zeros((rows, 1), jnp.int32)
    place1 = jnp.zeros((rows, 1), jnp.int32)
    for s in range(seqs):
        taken1 = jnp.where(row1 // steps == s, acc[s], taken1)
        place1 = jnp.where(row1 // steps == s, pos[s], place1)
    live = same & (col % steps < taken1)
    highest = lax.Precision.HIGHEST
    cum = -jnp.dot(tri.astype(jnp.float32), rate, precision=highest, preferred_element_type=jnp.float32)
    cum_taken = -jnp.dot(live.astype(jnp.float32), rate, precision=highest, preferred_element_type=jnp.float32)
    grown = jnp.exp(cum)
    grown_taken = jnp.exp(cum_taken)
    token = jnp.exp(jnp.minimum(cum_taken - cum, 0.0)) * (row1 % steps < taken1).astype(jnp.float32)
    head_lane = lax.broadcasted_iota(jnp.int32, (rows, plan.heads), 1)
    lane = lax.broadcasted_iota(jnp.int32, (rows, plan.count), 1)
    scale = None
    for i in range(plan.slots):
        hot = head_lane == lax.rem(first_head + i, plan.heads)

        def pick(values):
            return jnp.sum(jnp.where(hot, values, 0.0), axis=1, keepdims=True)

        taken_ref[i] = jnp.broadcast_to(pick(grown_taken), (rows, plan.width_n))
        decay_ref[i] = jnp.broadcast_to(pick(token), (rows, plan.width_p))
        wide = jnp.broadcast_to(pick(grown), (rows, plan.count))
        scale = wide if i == 0 else jnp.where(lane >= plan.starts[i], wide, scale)
        if i > 0:
            here = pick(cum)
            across = jnp.sum(jnp.where(row == col, here, 0.0), axis=0, keepdims=True)
            first = plan.starts[i]
            mix = jnp.where(tri, jnp.exp(jnp.minimum(here - across, 0.0)), 0.0)
            mix_ref[i - 1] = mix * weight[:, first : first + 1]
    occupied = jnp.right_shift(place1, (lane + plan.offset) % L) & 1
    factor = weight * occupied.astype(jnp.float32) * scale
    for s in range(seqs):
        for j in range(plan.count):
            column = factor[s * steps : (s + 1) * steps, j : j + 1]
            factor_ref[s, j] = jnp.broadcast_to(column, (steps, plan.width_n))
    for s in range(seqs):
        p, q = pos[s], pos[s] + acc[s]
        top = highest_bit(jnp.bitwise_xor(p, q))
        leaving = jnp.where(top >= plan.offset, p, 0)
        state_copies[s].wait()
        total = None
        for k in range(plan.offset):
            bit = (jnp.right_shift(leaving, k) & 1) * (k < top).astype(jnp.int32)
            term = states_ref[s, k] * bit.astype(jnp.float32)
            total = term if total is None else total + term
        fold_ref[s] = total.astype(fold_ref.dtype)


def assemble_kernel(plan, pair_ref, *refs):
    *far_refs, sums_ref, decay_ref, mix_ref, count_ref, counted_ref = refs[: plan.devices // 2 - 1 + 5]
    in_ref, out_ref, token_ref, draft_ref, send_ref, sum_ref, all_ref = refs[plan.devices // 2 - 1 + 5 :]
    sum_ref[...] = count_ref[...] + counted_ref[...]
    rows, shard = plan.rows, plan.shard
    me = lax.axis_index("level")
    for half, ref in enumerate([pair_ref, *far_refs]):
        for side in range(2):
            source = jnp.bitwise_xor(me, 2 * half + side)
            part = ref[side].astype(jnp.float32).reshape(rows, shard)
            all_ref[source] = part.astype(jnp.bfloat16)

    def features(first, width, pieces):
        k = lax.broadcasted_iota(jnp.int32, (shard, width), 0)
        c = lax.broadcasted_iota(jnp.int32, (shard, width), 1)
        total = None
        start = first // shard
        for piece in range(pieces):
            source = start + piece
            hot = (k + source * shard == c + first).astype(jnp.float32).astype(jnp.bfloat16)
            index = jnp.minimum(source, plan.devices - 1)
            term = jnp.dot(all_ref[index], hot, preferred_element_type=jnp.float32)
            total = term if total is None else total + term
        return total

    def pieces_of(width):
        return (width + shard - 2) // shard + 1

    in_vecs = features(plan.value_width, plan.width_n, pieces_of(plan.width_n))
    out_vecs = features(plan.value_width + plan.width_n, plan.width_n, pieces_of(plan.width_n))
    in_ref[...] = in_vecs
    out_ref[...] = out_vecs
    scores = dot_nt(out_vecs.astype(jnp.bfloat16), in_vecs.astype(jnp.bfloat16))
    drafts = []
    for i in range(plan.slots):
        head = lax.rem(me * plan.own + i, plan.heads)
        value = features(head * plan.width_p, plan.width_p, pieces_of(plan.width_p))
        token_ref[:, i * plan.width_p : (i + 1) * plan.width_p] = value * decay_ref[i]
        if i > 0:
            high, low = split(mix_ref[i - 1] * scores)
            value = value.astype(jnp.bfloat16)
            drafts.append(
                jnp.dot(high, value, preferred_element_type=jnp.float32)
                + jnp.dot(low, value, preferred_element_type=jnp.float32)
            )
        else:
            drafts.append(jnp.zeros((rows, plan.width_p), jnp.float32))
    draft_ref[...] = jnp.concatenate(drafts[:-1], axis=1)
    steps = plan.steps
    for s in range(plan.seqs):
        at = slice(s * steps, (s + 1) * steps)
        send_ref[at] = applied(sums_ref[s, plan.own], out_vecs[at]) + drafts[-1][at]


def base_kernel(plan, pos, acc, states_ref, factor_ref, taken_ref, new_hbm, sums_ref, low_ref, merged_ref, new_ref, sems):
    s = pl.program_id(0)
    steps, width_p, width_n, size = plan.steps, plan.width_p, plan.width_n, plan.offset
    parts = plan.count // size
    p = pos[s]
    q = p + acc[s]
    top = highest_bit(jnp.bitwise_xor(p, q))
    bound = jnp.maximum(top, 0)
    upto = jnp.where(top < 0, 0, jnp.left_shift(2, bound) - 1)
    staying = p & q & jnp.bitwise_not(upto)
    leaving = jnp.where(top < 0, 0, p & (jnp.left_shift(1, bound) - 1))
    side = lax.rem(s, 2)
    half = width_p // PARTS

    def sent(r, s, side):
        at = pl.ds(r * size, size)
        return pltpu.make_async_copy(new_ref.at[side, at], new_hbm.at[s, at], sems.at[side, r])

    @pl.loop(0, parts)
    def _(r):
        @pl.when(s >= 2)
        def _():
            sent(r, s - 2, side).wait()

        slot = jnp.right_shift(r + 1, 1)
        upper = 1 - (r & 1)
        more = (r > 0) & (upper == 1)
        stay = jnp.right_shift(staying, upper * size)
        leave = jnp.right_shift(leaving, upper * size)
        grown = taken_ref[slot, 0:1, :]
        for part in range(PARTS):
            at = slice(part * half, (part + 1) * half)
            sums = [jnp.where(more, sums_ref[0, slot, t, at, :], 0.0) for t in range(steps)]
            merged = jnp.where(more, merged_ref[0, slot, at, :], 0.0)
            for k in range(size):
                state = states_ref[0, r * size + k, at, :]
                kept = (jnp.right_shift(stay, k) & 1).astype(jnp.float32)
                new_ref[side, r * size + k, at, :] = state * (grown * kept)
                left = (jnp.right_shift(leave, k) & 1).astype(jnp.float32)
                merged = merged + state * left
                for t in range(steps):
                    sums[t] = sums[t] + state * factor_ref[0, r * size + k, t : t + 1, :]
            merged_ref[0, slot, at, :] = merged
            for t in range(steps):
                sums_ref[0, slot, t, at, :] = sums[t]

        @pl.when(upper == 0)
        def _():
            low_ref[0, slot - 1] = new_ref[side, pl.ds(r * size, plan.low)]

        sent(r, s, side).start()

    @pl.when(s == plan.seqs - 1)
    def _():
        for r in range(parts):
            sent(r, s - 1, 1 - side).wait()
            sent(r, s, side).wait()


def settle_kernel(plan, pos, acc, sums_ref, low_ref, merged_ref, taken_ref, in_ref, out_ref, token_ref,
                  draft_ref, fold_ref, old_hbm, new_hbm, own_ref, low_buf, top_buf, low_sems, top_sems):
    del old_hbm
    steps, width_p, width_n, low = plan.steps, plan.width_p, plan.width_n, plan.low
    step = lax.broadcasted_iota(jnp.int32, (2 * steps, width_n), 0) % steps
    copies = []
    for s in range(plan.seqs):
        rows = slice(s * steps, (s + 1) * steps)
        p = pos[s]
        a = acc[s]
        q = p + a
        top = highest_bit(jnp.bitwise_xor(p, q))
        bound = jnp.maximum(top, 0)
        in_vecs = in_ref[rows]
        in_twice = jnp.concatenate([in_vecs, in_vecs], axis=0)
        groups = []
        for g in range(low + 1):
            level = bound if g == low else g
            wanted = (jnp.right_shift(q, level) & 1) == 1
            if g < low:
                wanted = wanted & (top != g)
            start = jnp.left_shift(jnp.right_shift(q, level + 1), level + 1)
            last = jnp.minimum(start + jnp.left_shift(1, level) - p, a)
            last = jnp.where(wanted, last, 0)
            inside = (step >= start - p) & (step < last)
            groups.append(jnp.where(inside, in_twice, 0.0).astype(jnp.bfloat16))
        spread = jnp.concatenate(split(token_ref[rows]), axis=0)
        added = lax.dot_general(
            spread, jnp.concatenate(groups, axis=1), (((0,), (0,)), ((), ())),
            preferred_element_type=jnp.float32,
        )

        def tokens(i, g):
            return added[i * width_p : (i + 1) * width_p, g * width_n : (g + 1) * width_n]

        for i in range(plan.slots):
            grown = taken_ref[i, s * steps : s * steps + 1, :]
            merged = merged_ref[s, i]
            here = top >= 0
            if i == 0:
                here = top >= plan.offset
                merged = merged + fold_ref[s].astype(jnp.float32)
            if i == plan.own:
                here = here & (top < plan.offset)
            value = merged * grown + tokens(i, low)
            top_buf[s, i] = value
            base = plan.starts[i] - (plan.offset if i == 0 else 0)
            far = here & (top >= low)
            copy = pltpu.make_async_copy(
                top_buf.at[s, i], new_hbm.at[s, base + jnp.where(far, top, low)], top_sems.at[s, i]
            )
            copies.append((far, copy))
            pl.when(far)(copy.start)
            if i > 0:
                for g in range(low):
                    low_buf[s, i - 1, g] = low_ref[s, i - 1, g] + tokens(i, g)

                @pl.when(here & (top < low))
                def _():
                    low_buf[s, i - 1, bound] = value

                copy = pltpu.make_async_copy(
                    low_buf.at[s, i - 1], new_hbm.at[s, pl.ds(plan.starts[i], low)], low_sems.at[s, i - 1]
                )
                copies.append((None, copy))
                copy.start()
        query = out_ref[rows]
        for i in range(plan.own):
            at = slice(i * width_p, (i + 1) * width_p)
            own_ref[rows, at] = applied(sums_ref[s, i], query) + draft_ref[rows, at]
    for far, copy in copies:
        if far is None:
            copy.wait()
        else:
            pl.when(far)(copy.wait)


def finish_kernel(plan, scale, own_ref, received_ref, count_ref, counted_ref, out_ref, share_ref):
    width_p = plan.width_p
    own = own_ref[...]
    first = own[:, :width_p] + received_ref[...]
    total = jnp.concatenate([first, own[:, width_p:]], axis=1)
    out_ref[...] = total.reshape(out_ref.shape).astype(out_ref.dtype)
    share_ref[...] = ((count_ref[...] + counted_ref[...]) * scale)[:1, :1]


def whole(shape, index=None):
    zeros = (0,) * len(shape)
    return pl.BlockSpec(shape, lambda *_: index if index else zeros)


def fast_on_device(plan, states, xbc, rates, level_weights, positions, accepted):
    devices, seqs, steps, rows = plan.devices, plan.seqs, plan.steps, plan.rows
    count, slots, own = plan.count, plan.slots, plan.own
    width_p, width_n = plan.width_p, plan.width_n
    f32 = jnp.float32
    groups = lax.axis_size("seq")
    swap = lambda x, by: lax.ppermute(x, "level", [(i, i ^ by) for i in range(devices)])
    parts = count // plan.offset
    hbm = pl.BlockSpec(memory_space=pltpu.HBM)
    pair = jnp.stack([xbc, swap(xbc, 1)])
    far = [swap(pair, by) for by in range(2, devices, 2)]
    factor, taken, decay, mix, fold, counted = pl.pallas_call(
        functools.partial(tables_kernel, plan),
        grid=(1,),
        in_specs=[pl.BlockSpec(memory_space=pltpu.HBM)] * 5,
        out_specs=[whole((seqs, count, steps, width_n)), whole((slots, rows, width_n)), whole((slots, rows, width_p)),
                   whole((own, rows, rows)), whole((seqs, width_p, width_n)), whole((8, 128))],
        scratch_shapes=[
            pltpu.SMEM((seqs,), jnp.int32), pltpu.SMEM((seqs,), jnp.int32),
            pltpu.VMEM(rates.shape, f32), pltpu.VMEM(level_weights.shape, f32),
            pltpu.VMEM((seqs, plan.offset, width_p, width_n), f32),
            pltpu.SemaphoreType.DMA((4,)), pltpu.SemaphoreType.DMA((seqs,)),
        ],
        out_shape=[
            jax.ShapeDtypeStruct((seqs, count, steps, width_n), f32),
            jax.ShapeDtypeStruct((slots, rows, width_n), f32),
            jax.ShapeDtypeStruct((slots, rows, width_p), f32),
            jax.ShapeDtypeStruct((own, rows, rows), f32),
            jax.ShapeDtypeStruct((seqs, width_p, width_n), jnp.bfloat16),
            jax.ShapeDtypeStruct((8, 128), f32),
        ],
        compiler_params=pltpu.CompilerParams(vmem_limit_bytes=VMEM),
        cost_estimate=pl.CostEstimate(flops=2_000_000, bytes_accessed=3_000_000, transcendentals=0),
        name="tables",
    )(*[pltpu.with_memory_space_constraint(x, pltpu.HBM) for x in (positions, accepted, rates, level_weights, states)])
    fold_in = passed_along(fold, "level", 1)
    base_states, sums, low, merged = pl.pallas_call(
        functools.partial(base_kernel, plan),
        grid_spec=pltpu.PrefetchScalarGridSpec(
            num_scalar_prefetch=2, grid=(seqs,),
            in_specs=[
                pl.BlockSpec((1, count, width_p, width_n), lambda s, *_: (s, 0, 0, 0)),
                pl.BlockSpec((1, count, steps, width_n), lambda s, *_: (s, 0, 0, 0)),
                pl.BlockSpec((slots, steps, width_n), lambda s, *_: (0, s, 0)),
            ],
            out_specs=[
                hbm,
                pl.BlockSpec((1, slots, steps, width_p, width_n), lambda s, *_: (s, 0, 0, 0, 0)),
                pl.BlockSpec((1, own, plan.low, width_p, width_n), lambda s, *_: (s, 0, 0, 0, 0)),
                pl.BlockSpec((1, slots, width_p, width_n), lambda s, *_: (s, 0, 0, 0)),
            ],
            scratch_shapes=[
                pltpu.VMEM((2, count, width_p, width_n), f32),
                pltpu.SemaphoreType.DMA((2, parts)),
            ],
        ),
        out_shape=[
            jax.ShapeDtypeStruct(states.shape, f32),
            jax.ShapeDtypeStruct((seqs, slots, steps, width_p, width_n), f32),
            jax.ShapeDtypeStruct((seqs, own, plan.low, width_p, width_n), f32),
            jax.ShapeDtypeStruct((seqs, slots, width_p, width_n), f32),
        ],
        compiler_params=pltpu.CompilerParams(vmem_limit_bytes=BASE_VMEM),
        cost_estimate=pl.CostEstimate(flops=20_000_000, bytes_accessed=32_000_000, transcendentals=0),
        name="base",
    )(positions, accepted, states, factor, taken)
    meet = lambda x, by: lax.ppermute(x, "seq", [(i, i ^ by) for i in range(groups)])
    counted_in = meet(counted, 1)
    in_vecs, out_vecs, token, draft, send, summed = pl.pallas_call(
        functools.partial(assemble_kernel, plan),
        grid=(1,),
        in_specs=[whole(pair.shape)] * (1 + len(far)) + [
            whole(sums.shape), whole(decay.shape), whole(mix.shape),
            whole(counted.shape), whole(counted.shape)],
        out_specs=[whole((rows, width_n))] * 2 + [whole((rows, slots * width_p)), whole((rows, own * width_p)),
                                                  whole((rows, width_p)), whole(counted.shape)],
        out_shape=[jax.ShapeDtypeStruct((rows, width_n), f32)] * 2 + [
            jax.ShapeDtypeStruct((rows, slots * width_p), f32),
            jax.ShapeDtypeStruct((rows, own * width_p), f32),
            jax.ShapeDtypeStruct((rows, width_p), f32),
            jax.ShapeDtypeStruct(counted.shape, f32)],
        scratch_shapes=[pltpu.VMEM((devices, rows, plan.shard), jnp.bfloat16)],
        compiler_params=pltpu.CompilerParams(vmem_limit_bytes=VMEM),
        cost_estimate=pl.CostEstimate(flops=2_000_000, bytes_accessed=3_000_000, transcendentals=0),
        name="assemble",
    )(pair, *far, sums, decay, mix, counted, counted_in)
    by = 2
    while 2 * by < groups:
        summed = summed + meet(summed, by)
        by *= 2
    summed_in = meet(summed, by)
    received = passed_along(send, "level", 1)
    settled = [whole(sums.shape), whole(low.shape), whole(merged.shape), whole(taken.shape),
               whole(in_vecs.shape), whole(out_vecs.shape), whole(token.shape), whole(draft.shape), whole(fold.shape)]
    new_states, own_out = pl.pallas_call(
        functools.partial(settle_kernel, plan),
        grid_spec=pltpu.PrefetchScalarGridSpec(
            num_scalar_prefetch=2, grid=(1,),
            in_specs=settled + [hbm],
            out_specs=[hbm, whole((rows, own * width_p))],
            scratch_shapes=[
                pltpu.VMEM(low.shape, f32), pltpu.VMEM(merged.shape, f32),
                pltpu.SemaphoreType.DMA((seqs, own)), pltpu.SemaphoreType.DMA((seqs, slots)),
            ],
        ),
        out_shape=[
            jax.ShapeDtypeStruct(states.shape, f32),
            jax.ShapeDtypeStruct((rows, own * width_p), f32),
        ],
        input_output_aliases={2 + len(settled): 0},
        compiler_params=pltpu.CompilerParams(vmem_limit_bytes=VMEM),
        cost_estimate=pl.CostEstimate(flops=8_000_000, bytes_accessed=8_000_000, transcendentals=0),
        name="settle",
    )(positions, accepted, sums, low, merged, taken, in_vecs, out_vecs, token, draft, fold_in, base_states)
    outputs, share = pl.pallas_call(
        functools.partial(finish_kernel, plan, 1.0 / (groups * seqs * steps)),
        grid=(1,),
        in_specs=[whole((rows, own * width_p)), whole((rows, width_p)), whole(counted.shape), whole(counted.shape)],
        out_specs=[whole((seqs, steps, own * width_p)), whole((1, 1))],
        out_shape=[jax.ShapeDtypeStruct((seqs, steps, own * width_p), jnp.bfloat16),
                   jax.ShapeDtypeStruct((1, 1), f32)],
        compiler_params=pltpu.CompilerParams(vmem_limit_bytes=VMEM),
        name="finish",
    )(own_out, received, summed, summed_in)
    return outputs, new_states, share.reshape(())


def dispatch(states, xbc, rates, level_weights, positions, accepted):
    plan = Plan(lax.axis_size("level"), states, xbc, rates)
    step = functools.partial(fast_on_device, plan) if plan.fits(lax.axis_size("seq")) else on_device
    return step(states, xbc, rates, level_weights, positions, accepted)


def solution(mesh):
    in_specs = (
        P("seq", "level", None, None),
        P("seq", None, "level"),
        P("seq", None, None),
        P("seq", None, "level"),
        P("seq"),
        P("seq"),
    )
    out_specs = (P("seq", None, "level"), P("seq", "level", None, None), P())
    return jax.shard_map(
        dispatch, mesh=mesh, in_specs=in_specs, out_specs=out_specs, check_vma=False
    )
```

```python
import functools

import jax
import jax.numpy as jnp
from jax import lax
from jax.experimental import pallas as pl
from jax.experimental.pallas import tpu as pltpu
from jax.sharding import PartitionSpec as P

H = 24
P_SIZE = 64
N = 128
L = 20
K = 8
PARTS = 4
VMEM = 24 * 2**20
BASE_VMEM = 20 * 2**20


def passed_along(x, axis, by):
    devices = lax.axis_size(axis)
    return lax.ppermute(x, axis, [(i, (i + by) % devices) for i in range(devices)])


def on_device(states, xbc, rates, level_weights, positions, accepted):
    highest = lax.Precision.HIGHEST
    seqs_local, local_count, width_p, width_n = states.shape
    offset = L // 2
    total_entries = H * L
    gathered = lax.all_gather(xbc, "level", axis=2, tiled=True).astype(jnp.float32)
    values = gathered[:, :, : H * P_SIZE].reshape(seqs_local, K, H, P_SIZE)
    in_vecs = gathered[:, :, H * P_SIZE : H * P_SIZE + N]
    out_vecs = gathered[:, :, H * P_SIZE + N :]
    cumul = jnp.cumsum(-rates, axis=1)
    first_entry = lax.axis_index("level") * local_count
    entries = first_entry + jnp.arange(local_count, dtype=jnp.int32)
    global_ids = (entries + offset) % total_entries
    head_of = global_ids // L
    level_of = global_ids % L
    head_ids = jnp.arange(H, dtype=jnp.int32)
    select = (head_of[:, None] == head_ids[None, :]).astype(jnp.float32)
    occupied = (jnp.right_shift(positions[:, None], level_of[None, :]) % 2).astype(jnp.float32)
    cum_local = jnp.einsum("sth,jh->stj", cumul, select, precision=highest)
    readout = jnp.einsum("sjpn,stn->stjp", states, out_vecs, precision=highest)
    factor = level_weights * occupied[:, None, :] * jnp.exp(cum_local)
    steps_all = jnp.arange(K, dtype=jnp.int32)
    causal = steps_all[None, :] <= steps_all[:, None]
    scores = jnp.einsum("stn,sun->stu", out_vecs, in_vecs, precision=highest)
    spread = cumul[:, :, None, :] - cumul[:, None, :, :]
    mixing = (
        jnp.where(causal[None, :, :, None], jnp.exp(jnp.minimum(spread, 0.0)), 0.0)
        * scores[..., None]
    )
    is_first = (level_of == 0).astype(jnp.float32)
    devices = lax.axis_size("level")
    own_width = H * P_SIZE // devices
    most_heads = 1
    distances = []
    for sender in range(devices):
        start_global = (sender * local_count + offset) % total_entries
        head_low = start_global // L
        head_count = (start_global + local_count - 1) // L - head_low + 1
        most_heads = max(most_heads, head_count)
        for slot_index in range(head_count):
            head_now = (head_low + slot_index) % H
            for receiver in range(
                head_now * P_SIZE // own_width, ((head_now + 1) * P_SIZE - 1) // own_width + 1
            ):
                gap = (receiver - sender) % devices
                if gap > devices // 2:
                    gap = gap - devices
                if gap != 0 and gap not in distances:
                    distances.append(gap)
    first_head = (first_entry + offset) % total_entries // L
    slot_heads = (first_head + jnp.arange(most_heads, dtype=jnp.int32)) % H
    select_slot = (head_of[:, None] == slot_heads[None, :]).astype(jnp.float32)
    pick_head = (head_ids[:, None] == slot_heads[None, :]).astype(jnp.float32)
    states_slot = jnp.einsum("stj,stjp,ji->stip", factor, readout, select_slot, precision=highest)
    weight_slot = jnp.einsum(
        "stj,ji->sti", level_weights, select_slot * is_first[:, None], precision=highest
    )
    mixing_slot = jnp.einsum("stuh,hi->stui", mixing, pick_head, precision=highest)
    values_slot = jnp.einsum("suhp,hi->suip", values, pick_head, precision=highest)
    drafts_slot = weight_slot[..., None] * jnp.einsum(
        "stui,suip->stip", mixing_slot, values_slot, precision=highest
    )
    flat_slot = (states_slot + drafts_slot).reshape(seqs_local, K, most_heads * P_SIZE)

    def toward(distance):
        receiver_now = (lax.axis_index("level") + distance) % devices
        feature_ids = receiver_now * own_width + jnp.arange(own_width, dtype=jnp.int32)
        slot_of = (feature_ids // P_SIZE - first_head) % H
        valid = (slot_of < most_heads).astype(jnp.float32)
        offsets = jnp.clip(slot_of * P_SIZE + feature_ids % P_SIZE, 0, most_heads * P_SIZE - 1)
        picked = jnp.take(flat_slot, offsets, axis=2)
        return picked * valid[None, None, :]

    summed = toward(0)
    for distance in distances:
        summed = summed + passed_along(toward(distance), "level", distance)
    outputs = summed.astype(jnp.bfloat16)
    new_position = positions + accepted
    levels_all = jnp.arange(L, dtype=jnp.int32)
    changed = jnp.bitwise_xor(positions, new_position)
    top_level = (
        jnp.sum(
            (jnp.right_shift(changed[:, None], levels_all[None, :]) > 0).astype(jnp.int32), axis=1
        )
        - 1
    )
    staying = occupied * (level_of[None, :] > top_level[:, None]).astype(jnp.float32)
    leaving = occupied * (level_of[None, :] < top_level[:, None]).astype(jnp.float32)
    target = (level_of[None, :] == top_level[:, None]).astype(jnp.float32)
    reach = min(devices - 1, (L - 2 + local_count) // local_count)
    same_head = (head_of[:, None] == head_of[None, :]).astype(jnp.float32)
    incoming = jnp.einsum("ab,sb,sbpn->sapn", same_head, leaving, states, precision=highest)
    place = target * (head_of == first_head).astype(jnp.float32)[None, :]
    for distance in range(1, reach + 1):
        receiver_start = (first_entry + distance * local_count + offset) % total_entries
        receiver_head = receiver_start // L
        target_global = receiver_head * L + top_level
        in_range = (
            (target_global >= receiver_start) & (target_global < receiver_start + local_count)
        ).astype(jnp.float32)
        pick_mask = (
            leaving * (head_of == receiver_head).astype(jnp.float32)[None, :] * in_range[:, None]
        )
        folded_sum = jnp.einsum("sj,sjpn->spn", pick_mask, states, precision=highest)
        received = passed_along(folded_sum.astype(jnp.bfloat16), "level", distance).astype(
            folded_sum.dtype
        )
        incoming = incoming + place[:, :, None, None] * received[:, None]
    merged = staying[:, :, None, None] * states + target[:, :, None, None] * incoming
    new_occ = (jnp.right_shift(new_position[:, None], level_of[None, :]) % 2).astype(jnp.float32)
    live = (steps_all[None, :] < accepted[:, None]).astype(jnp.float32)
    cum_taken = jnp.sum(-rates * live[:, :, None], axis=1)
    taken_local = jnp.einsum("sh,jh->sj", cum_taken, select, precision=highest)
    token_pos = positions[:, None] + steps_all[None, :]
    start_new = jnp.left_shift(
        jnp.right_shift(new_position[:, None], level_of[None, :] + 1), level_of[None, :] + 1
    )
    level_span = jnp.left_shift(jnp.int32(1), level_of)
    inside = (
        (token_pos[:, None, :] >= start_new[:, :, None])
        & (token_pos[:, None, :] < start_new[:, :, None] + level_span[None, :, None])
    ).astype(jnp.float32) * live[:, None, :]
    token_decay = jnp.exp(jnp.minimum(taken_local[:, None, :] - cum_local, 0.0)) * live[:, :, None]
    values_local = jnp.einsum("suhp,jh->sujp", values, select, precision=highest)
    tokens = jnp.einsum(
        "sju,suj,sujp,sun->sjpn", inside, token_decay, values_local, in_vecs, precision=highest
    )
    new_states = new_occ[:, :, None, None] * (
        jnp.exp(taken_local)[:, :, None, None] * merged + tokens
    )
    total_taken = lax.psum(jnp.sum(accepted.astype(jnp.float32)), "seq")
    acceptance = total_taken / (lax.axis_size("seq") * seqs_local * K)
    return (outputs, new_states, acceptance)


def highest_bit(value):
    return 31 - lax.clz(value)


def split(value):
    high = value.astype(jnp.bfloat16)
    low = (value - high.astype(jnp.float32)).astype(jnp.bfloat16)
    return high, low


def dot_nt(left, right):
    return lax.dot_general(
        left, right, (((1,), (1,)), ((), ())), preferred_element_type=jnp.float32
    )


def applied(sums, queries):
    lane = lax.broadcasted_iota(jnp.int32, (sums.shape[1], queries.shape[0]), 1)
    total = None
    for t in range(queries.shape[0]):
        term = jnp.sum(sums[t] * queries[t : t + 1, :], axis=1, keepdims=True)
        total = jnp.broadcast_to(term, lane.shape) if t == 0 else jnp.where(lane == t, term, total)
    return total.T


class Plan:
    def __init__(self, devices, states, xbc, rates):
        self.seqs, self.count, self.width_p, self.width_n = states.shape
        self.steps = xbc.shape[1]
        self.shard = xbc.shape[2]
        self.heads = rates.shape[2]
        self.devices = devices
        self.offset = L // 2
        self.own = self.count // L
        self.slots = self.own + 1
        self.rows = self.seqs * self.steps
        self.low = (self.steps - 1).bit_length()
        self.starts = [0] + [L - self.offset + i * L for i in range(self.own)] + [self.count]
        self.value_width = self.heads * self.width_p

    def fits(self, groups):
        return (
            self.count % L == 0
            and L - self.offset == self.offset
            and self.devices & (self.devices - 1) == 0
            and self.devices > 1
            and self.heads == self.own * self.devices
            and self.steps == 8
            and self.seqs > 1
            and groups >= 4
            and groups & (groups - 1) == 0
            and self.low <= self.offset
        )

    def levels(self, slot):
        first = self.offset if slot == 0 else 0
        return [(j, first + j - self.starts[slot]) for j in range(self.starts[slot], self.starts[slot + 1])]


def tables_kernel(plan, pos_hbm, acc_hbm, rates_hbm, weights_hbm, states_hbm, factor_ref, taken_ref,
                  decay_ref, mix_ref, fold_ref, count_ref, pos, acc, rates_ref, weights_ref, states_ref, sems, state_sems):
    copies = [
        pltpu.make_async_copy(source, target, sems.at[n])
        for n, (source, target) in enumerate(
            [(pos_hbm, pos), (acc_hbm, acc), (rates_hbm, rates_ref), (weights_hbm, weights_ref)]
        )
    ]
    state_copies = [
        pltpu.make_async_copy(
            states_hbm.at[s, pl.ds(plan.count - plan.offset, plan.offset)], states_ref.at[s], state_sems.at[s]
        )
        for s in range(plan.seqs)
    ]
    for copy in copies + state_copies:
        copy.start()
    for copy in copies:
        copy.wait()
    rows, steps, seqs = plan.rows, plan.steps, plan.seqs
    first_head = lax.axis_index("level") * plan.own
    count_ref[...] = jnp.full(count_ref.shape, sum(acc[s] for s in range(seqs)).astype(jnp.float32))
    rate = rates_ref[...].reshape(rows, plan.heads)
    weight = weights_ref[...].reshape(rows, plan.count)
    row = lax.broadcasted_iota(jnp.int32, (rows, rows), 0)
    col = lax.broadcasted_iota(jnp.int32, (rows, rows), 1)
    same = row // steps == col // steps
    tri = same & (col <= row)
    row1 = lax.broadcasted_iota(jnp.int32, (rows, 1), 0)
    taken1 = jnp.zeros((rows, 1), jnp.int32)
    place1 = jnp.zeros((rows, 1), jnp.int32)
    for s in range(seqs):
        taken1 = jnp.where(row1 // steps == s, acc[s], taken1)
        place1 = jnp.where(row1 // steps == s, pos[s], place1)
    live = same & (col % steps < taken1)
    highest = lax.Precision.HIGHEST
    cum = -jnp.dot(tri.astype(jnp.float32), rate, precision=highest, preferred_element_type=jnp.float32)
    cum_taken = -jnp.dot(live.astype(jnp.float32), rate, precision=highest, preferred_element_type=jnp.float32)
    grown = jnp.exp(cum)
    grown_taken = jnp.exp(cum_taken)
    token = jnp.exp(jnp.minimum(cum_taken - cum, 0.0)) * (row1 % steps < taken1).astype(jnp.float32)
    head_lane = lax.broadcasted_iota(jnp.int32, (rows, plan.heads), 1)
    lane = lax.broadcasted_iota(jnp.int32, (rows, plan.count), 1)
    scale = None
    for i in range(plan.slots):
        hot = head_lane == lax.rem(first_head + i, plan.heads)

        def pick(values):
            return jnp.sum(jnp.where(hot, values, 0.0), axis=1, keepdims=True)

        taken_ref[i] = jnp.broadcast_to(pick(grown_taken), (rows, plan.width_n))
        decay_ref[i] = jnp.broadcast_to(pick(token), (rows, plan.width_p))
        wide = jnp.broadcast_to(pick(grown), (rows, plan.count))
        scale = wide if i == 0 else jnp.where(lane >= plan.starts[i], wide, scale)
        if i > 0:
            here = pick(cum)
            across = jnp.sum(jnp.where(row == col, here, 0.0), axis=0, keepdims=True)
            first = plan.starts[i]
            mix = jnp.where(tri, jnp.exp(jnp.minimum(here - across, 0.0)), 0.0)
            mix_ref[i - 1] = mix * weight[:, first : first + 1]
    occupied = jnp.right_shift(place1, (lane + plan.offset) % L) & 1
    factor = weight * occupied.astype(jnp.float32) * scale
    for s in range(seqs):
        for j in range(plan.count):
            column = factor[s * steps : (s + 1) * steps, j : j + 1]
            factor_ref[s, j] = jnp.broadcast_to(column, (steps, plan.width_n))
    for s in range(seqs):
        p, q = pos[s], pos[s] + acc[s]
        changed = jnp.right_shift(jnp.bitwise_xor(p, q), plan.offset)
        leaving = jnp.where(changed > 0, p, 0)
        state_copies[s].wait()
        total = None
        for k in range(plan.offset):
            bit = jnp.right_shift(leaving, k) & 1
            term = states_ref[s, k] * bit.astype(jnp.float32)
            total = term if total is None else total + term
        fold_ref[s] = total.astype(fold_ref.dtype)


def assemble_kernel(plan, pair_ref, *refs):
    *far_refs, sums_ref, decay_ref, mix_ref, count_ref, counted_ref = refs[: plan.devices // 2 - 1 + 5]
    in_ref, out_ref, token_ref, draft_ref, send_ref, sum_ref, all_ref = refs[plan.devices // 2 - 1 + 5 :]
    sum_ref[...] = count_ref[...] + counted_ref[...]
    rows, shard = plan.rows, plan.shard
    me = lax.axis_index("level")
    for half, ref in enumerate([pair_ref, *far_refs]):
        for side in range(2):
            source = jnp.bitwise_xor(me, 2 * half + side)
            part = ref[side].astype(jnp.float32).reshape(rows, shard)
            all_ref[source] = part.astype(jnp.bfloat16)

    def features(first, width, pieces):
        k = lax.broadcasted_iota(jnp.int32, (shard, width), 0)
        c = lax.broadcasted_iota(jnp.int32, (shard, width), 1)
        total = None
        start = first // shard
        for piece in range(pieces):
            source = start + piece
            hot = (k + source * shard == c + first).astype(jnp.float32).astype(jnp.bfloat16)
            index = jnp.minimum(source, plan.devices - 1)
            term = jnp.dot(all_ref[index], hot, preferred_element_type=jnp.float32)
            total = term if total is None else total + term
        return total

    def pieces_of(width):
        return (width + shard - 2) // shard + 1

    in_vecs = features(plan.value_width, plan.width_n, pieces_of(plan.width_n))
    out_vecs = features(plan.value_width + plan.width_n, plan.width_n, pieces_of(plan.width_n))
    in_ref[...] = in_vecs
    out_ref[...] = out_vecs
    scores = dot_nt(out_vecs.astype(jnp.bfloat16), in_vecs.astype(jnp.bfloat16))
    drafts = []
    for i in range(plan.slots):
        head = lax.rem(me * plan.own + i, plan.heads)
        value = features(head * plan.width_p, plan.width_p, pieces_of(plan.width_p))
        token_ref[:, i * plan.width_p : (i + 1) * plan.width_p] = value * decay_ref[i]
        if i > 0:
            high, low = split(mix_ref[i - 1] * scores)
            value = value.astype(jnp.bfloat16)
            drafts.append(
                jnp.dot(high, value, preferred_element_type=jnp.float32)
                + jnp.dot(low, value, preferred_element_type=jnp.float32)
            )
        else:
            drafts.append(jnp.zeros((rows, plan.width_p), jnp.float32))
    draft_ref[...] = jnp.concatenate(drafts[:-1], axis=1)
    steps = plan.steps
    for s in range(plan.seqs):
        at = slice(s * steps, (s + 1) * steps)
        send_ref[at] = applied(sums_ref[s, plan.own], out_vecs[at]) + drafts[-1][at]


def base_kernel(plan, pos, acc, states_ref, factor_ref, taken_ref, new_hbm, sums_ref, low_ref, merged_ref, new_ref, sems):
    s = pl.program_id(0)
    steps, width_p, width_n, size = plan.steps, plan.width_p, plan.width_n, plan.offset
    parts = plan.count // size
    p = pos[s]
    q = p + acc[s]
    top = highest_bit(jnp.bitwise_xor(p, q))
    bound = jnp.maximum(top, 0)
    upto = jnp.where(top < 0, 0, jnp.left_shift(2, bound) - 1)
    staying = p & q & jnp.bitwise_not(upto)
    leaving = jnp.where(top < 0, 0, p & (jnp.left_shift(1, bound) - 1))
    side = lax.rem(s, 2)
    half = width_p // PARTS

    def sent(r, s, side):
        at = pl.ds(r * size, size)
        return pltpu.make_async_copy(new_ref.at[side, at], new_hbm.at[s, at], sems.at[side, r])

    @pl.loop(0, parts)
    def _(r):
        @pl.when(s >= 2)
        def _():
            sent(r, s - 2, side).wait()

        slot = jnp.right_shift(r + 1, 1)
        upper = 1 - (r & 1)
        more = (r > 0) & (upper == 1)
        stay = jnp.right_shift(staying, upper * size)
        leave = jnp.right_shift(leaving, upper * size)
        grown = taken_ref[slot, 0:1, :]
        for part in range(PARTS):
            at = slice(part * half, (part + 1) * half)
            sums = [jnp.where(more, sums_ref[0, slot, t, at, :], 0.0) for t in range(steps)]
            merged = jnp.where(more, merged_ref[0, slot, at, :], 0.0)
            for k in range(size):
                state = states_ref[0, r * size + k, at, :]
                kept = (jnp.right_shift(stay, k) & 1).astype(jnp.float32)
                new_ref[side, r * size + k, at, :] = state * (grown * kept)
                left = (jnp.right_shift(leave, k) & 1).astype(jnp.float32)
                merged = merged + state * left
                for t in range(steps):
                    sums[t] = sums[t] + state * factor_ref[0, r * size + k, t : t + 1, :]
            merged_ref[0, slot, at, :] = merged
            for t in range(steps):
                sums_ref[0, slot, t, at, :] = sums[t]

        @pl.when(upper == 0)
        def _():
            low_ref[0, slot - 1] = new_ref[side, pl.ds(r * size, plan.low)]

        sent(r, s, side).start()

    @pl.when(s == plan.seqs - 1)
    def _():
        for r in range(parts):
            sent(r, s - 1, 1 - side).wait()
            sent(r, s, side).wait()


def settle_kernel(plan, pos, acc, sums_ref, low_ref, merged_ref, taken_ref, in_ref, out_ref, token_ref,
                  draft_ref, fold_ref, old_hbm, new_hbm, own_ref, low_buf, top_buf, low_sems, top_sems):
    del old_hbm
    steps, width_p, width_n, low = plan.steps, plan.width_p, plan.width_n, plan.low
    step = lax.broadcasted_iota(jnp.int32, (2 * steps, width_n), 0) % steps
    copies = []
    for s in range(plan.seqs):
        rows = slice(s * steps, (s + 1) * steps)
        p = pos[s]
        a = acc[s]
        q = p + a
        top = highest_bit(jnp.bitwise_xor(p, q))
        bound = jnp.maximum(top, 0)
        in_vecs = in_ref[rows]
        in_twice = jnp.concatenate([in_vecs, in_vecs], axis=0)
        groups = []
        for g in range(low + 1):
            level = bound if g == low else g
            wanted = (jnp.right_shift(q, level) & 1) == 1
            if g < low:
                wanted = wanted & (top != g)
            start = jnp.left_shift(jnp.right_shift(q, level + 1), level + 1)
            last = jnp.minimum(start + jnp.left_shift(1, level) - p, a)
            last = jnp.where(wanted, last, 0)
            inside = (step >= start - p) & (step < last)
            groups.append(jnp.where(inside, in_twice, 0.0).astype(jnp.bfloat16))
        spread = jnp.concatenate(split(token_ref[rows]), axis=0)
        added = lax.dot_general(
            spread, jnp.concatenate(groups, axis=1), (((0,), (0,)), ((), ())),
            preferred_element_type=jnp.float32,
        )

        def tokens(i, g):
            return added[i * width_p : (i + 1) * width_p, g * width_n : (g + 1) * width_n]

        for i in range(plan.slots):
            grown = taken_ref[i, s * steps : s * steps + 1, :]
            merged = merged_ref[s, i]
            here = top >= 0
            if i == 0:
                here = top >= plan.offset
                merged = merged + fold_ref[s].astype(jnp.float32)
            if i == plan.own:
                here = here & (top < plan.offset)
            value = merged * grown + tokens(i, low)
            top_buf[s, i] = value
            base = plan.starts[i] - (plan.offset if i == 0 else 0)
            far = here & (top >= low)
            copy = pltpu.make_async_copy(
                top_buf.at[s, i], new_hbm.at[s, base + jnp.where(far, top, low)], top_sems.at[s, i]
            )
            copies.append((far, copy))
            pl.when(far)(copy.start)
            if i > 0:
                for g in range(low):
                    low_buf[s, i - 1, g] = low_ref[s, i - 1, g] + tokens(i, g)

                @pl.when(here & (top < low))
                def _():
                    low_buf[s, i - 1, bound] = value

                copy = pltpu.make_async_copy(
                    low_buf.at[s, i - 1], new_hbm.at[s, pl.ds(plan.starts[i], low)], low_sems.at[s, i - 1]
                )
                copies.append((None, copy))
                copy.start()
        query = out_ref[rows]
        for i in range(plan.own):
            at = slice(i * width_p, (i + 1) * width_p)
            own_ref[rows, at] = applied(sums_ref[s, i], query) + draft_ref[rows, at]
    for far, copy in copies:
        if far is None:
            copy.wait()
        else:
            pl.when(far)(copy.wait)


def finish_kernel(plan, scale, own_ref, received_ref, count_ref, counted_ref, out_ref, share_ref):
    width_p = plan.width_p
    own = own_ref[...]
    first = own[:, :width_p] + received_ref[...]
    total = jnp.concatenate([first, own[:, width_p:]], axis=1)
    out_ref[...] = total.reshape(out_ref.shape).astype(out_ref.dtype)
    share_ref[...] = ((count_ref[...] + counted_ref[...]) * scale)[:1, :1]


def whole(shape, index=None):
    zeros = (0,) * len(shape)
    return pl.BlockSpec(shape, lambda *_: index if index else zeros)


def fast_on_device(plan, states, xbc, rates, level_weights, positions, accepted):
    devices, seqs, steps, rows = plan.devices, plan.seqs, plan.steps, plan.rows
    count, slots, own = plan.count, plan.slots, plan.own
    width_p, width_n = plan.width_p, plan.width_n
    f32 = jnp.float32
    groups = lax.axis_size("seq")
    swap = lambda x, by: lax.ppermute(x, "level", [(i, i ^ by) for i in range(devices)])
    parts = count // plan.offset
    hbm = pl.BlockSpec(memory_space=pltpu.HBM)
    pair = jnp.stack([xbc, swap(xbc, 1)])
    far = [swap(pair, by) for by in range(2, devices, 2)]
    factor, taken, decay, mix, fold, counted = pl.pallas_call(
        functools.partial(tables_kernel, plan),
        grid=(1,),
        in_specs=[pl.BlockSpec(memory_space=pltpu.HBM)] * 5,
        out_specs=[whole((seqs, count, steps, width_n)), whole((slots, rows, width_n)), whole((slots, rows, width_p)),
                   whole((own, rows, rows)), whole((seqs, width_p, width_n)), whole((8, 128))],
        scratch_shapes=[
            pltpu.SMEM((seqs,), jnp.int32), pltpu.SMEM((seqs,), jnp.int32),
            pltpu.VMEM(rates.shape, f32), pltpu.VMEM(level_weights.shape, f32),
            pltpu.VMEM((seqs, plan.offset, width_p, width_n), f32),
            pltpu.SemaphoreType.DMA((4,)), pltpu.SemaphoreType.DMA((seqs,)),
        ],
        out_shape=[
            jax.ShapeDtypeStruct((seqs, count, steps, width_n), f32),
            jax.ShapeDtypeStruct((slots, rows, width_n), f32),
            jax.ShapeDtypeStruct((slots, rows, width_p), f32),
            jax.ShapeDtypeStruct((own, rows, rows), f32),
            jax.ShapeDtypeStruct((seqs, width_p, width_n), jnp.bfloat16),
            jax.ShapeDtypeStruct((8, 128), f32),
        ],
        compiler_params=pltpu.CompilerParams(vmem_limit_bytes=VMEM),
        cost_estimate=pl.CostEstimate(flops=2_000_000, bytes_accessed=3_000_000, transcendentals=0),
        name="tables",
    )(*[pltpu.with_memory_space_constraint(x, pltpu.HBM) for x in (positions, accepted, rates, level_weights, states)])
    fold_in = passed_along(fold, "level", 1)
    base_states, sums, low, merged = pl.pallas_call(
        functools.partial(base_kernel, plan),
        grid_spec=pltpu.PrefetchScalarGridSpec(
            num_scalar_prefetch=2, grid=(seqs,),
            in_specs=[
                pl.BlockSpec((1, count, width_p, width_n), lambda s, *_: (s, 0, 0, 0)),
                pl.BlockSpec((1, count, steps, width_n), lambda s, *_: (s, 0, 0, 0)),
                pl.BlockSpec((slots, steps, width_n), lambda s, *_: (0, s, 0)),
            ],
            out_specs=[
                hbm,
                pl.BlockSpec((1, slots, steps, width_p, width_n), lambda s, *_: (s, 0, 0, 0, 0)),
                pl.BlockSpec((1, own, plan.low, width_p, width_n), lambda s, *_: (s, 0, 0, 0, 0)),
                pl.BlockSpec((1, slots, width_p, width_n), lambda s, *_: (s, 0, 0, 0)),
            ],
            scratch_shapes=[
                pltpu.VMEM((2, count, width_p, width_n), f32),
                pltpu.SemaphoreType.DMA((2, parts)),
            ],
        ),
        out_shape=[
            jax.ShapeDtypeStruct(states.shape, f32),
            jax.ShapeDtypeStruct((seqs, slots, steps, width_p, width_n), f32),
            jax.ShapeDtypeStruct((seqs, own, plan.low, width_p, width_n), f32),
            jax.ShapeDtypeStruct((seqs, slots, width_p, width_n), f32),
        ],
        compiler_params=pltpu.CompilerParams(vmem_limit_bytes=BASE_VMEM),
        cost_estimate=pl.CostEstimate(flops=20_000_000, bytes_accessed=32_000_000, transcendentals=0),
        name="base",
    )(positions, accepted, states, factor, taken)
    meet = lambda x, by: lax.ppermute(x, "seq", [(i, i ^ by) for i in range(groups)])
    counted_in = meet(counted, 1)
    in_vecs, out_vecs, token, draft, send, summed = pl.pallas_call(
        functools.partial(assemble_kernel, plan),
        grid=(1,),
        in_specs=[whole(pair.shape)] * (1 + len(far)) + [
            whole(sums.shape), whole(decay.shape), whole(mix.shape),
            whole(counted.shape), whole(counted.shape)],
        out_specs=[whole((rows, width_n))] * 2 + [whole((rows, slots * width_p)), whole((rows, own * width_p)),
                                                  whole((rows, width_p)), whole(counted.shape)],
        out_shape=[jax.ShapeDtypeStruct((rows, width_n), f32)] * 2 + [
            jax.ShapeDtypeStruct((rows, slots * width_p), f32),
            jax.ShapeDtypeStruct((rows, own * width_p), f32),
            jax.ShapeDtypeStruct((rows, width_p), f32),
            jax.ShapeDtypeStruct(counted.shape, f32)],
        scratch_shapes=[pltpu.VMEM((devices, rows, plan.shard), jnp.bfloat16)],
        compiler_params=pltpu.CompilerParams(vmem_limit_bytes=VMEM),
        cost_estimate=pl.CostEstimate(flops=2_000_000, bytes_accessed=3_000_000, transcendentals=0),
        name="assemble",
    )(pair, *far, sums, decay, mix, counted, counted_in)
    by = 2
    while 2 * by < groups:
        summed = summed + meet(summed, by)
        by *= 2
    summed_in = meet(summed, by)
    received = passed_along(send, "level", 1)
    settled = [whole(sums.shape), whole(low.shape), whole(merged.shape), whole(taken.shape),
               whole(in_vecs.shape), whole(out_vecs.shape), whole(token.shape), whole(draft.shape), whole(fold.shape)]
    new_states, own_out = pl.pallas_call(
        functools.partial(settle_kernel, plan),
        grid_spec=pltpu.PrefetchScalarGridSpec(
            num_scalar_prefetch=2, grid=(1,),
            in_specs=settled + [hbm],
            out_specs=[hbm, whole((rows, own * width_p))],
            scratch_shapes=[
                pltpu.VMEM(low.shape, f32), pltpu.VMEM(merged.shape, f32),
                pltpu.SemaphoreType.DMA((seqs, own)), pltpu.SemaphoreType.DMA((seqs, slots)),
            ],
        ),
        out_shape=[
            jax.ShapeDtypeStruct(states.shape, f32),
            jax.ShapeDtypeStruct((rows, own * width_p), f32),
        ],
        input_output_aliases={2 + len(settled): 0},
        compiler_params=pltpu.CompilerParams(vmem_limit_bytes=VMEM),
        cost_estimate=pl.CostEstimate(flops=8_000_000, bytes_accessed=8_000_000, transcendentals=0),
        name="settle",
    )(positions, accepted, sums, low, merged, taken, in_vecs, out_vecs, token, draft, fold_in, base_states)
    outputs, share = pl.pallas_call(
        functools.partial(finish_kernel, plan, 1.0 / (groups * seqs * steps)),
        grid=(1,),
        in_specs=[whole((rows, own * width_p)), whole((rows, width_p)), whole(counted.shape), whole(counted.shape)],
        out_specs=[whole((seqs, steps, own * width_p)), whole((1, 1))],
        out_shape=[jax.ShapeDtypeStruct((seqs, steps, own * width_p), jnp.bfloat16),
                   jax.ShapeDtypeStruct((1, 1), f32)],
        compiler_params=pltpu.CompilerParams(vmem_limit_bytes=VMEM),
        name="finish",
    )(own_out, received, summed, summed_in)
    return outputs, new_states, share.reshape(())


def dispatch(states, xbc, rates, level_weights, positions, accepted):
    plan = Plan(lax.axis_size("level"), states, xbc, rates)
    step = functools.partial(fast_on_device, plan) if plan.fits(lax.axis_size("seq")) else on_device
    return step(states, xbc, rates, level_weights, positions, accepted)


def solution(mesh):
    in_specs = (
        P("seq", "level", None, None),
        P("seq", None, "level"),
        P("seq", None, None),
        P("seq", None, "level"),
        P("seq"),
        P("seq"),
    )
    out_specs = (P("seq", None, "level"), P("seq", "level", None, None), P())
    return jax.shard_map(
        dispatch, mesh=mesh, in_specs=in_specs, out_specs=out_specs, check_vma=False
    )
```
